32 devices in a mesh: fsdp: 8 (over y, x, core), seq: 4 (over z).
Axes of the slice: x: 2, y: 2, z: 4, core: 2. Of those that a mesh axis runs over, the one named last changes fastest.
Arguments:
- query_rows: bfloat16 [16, 768, 16, 128], P('fsdp', 'seq'), may hold values from -6 to 6
- key_rows: bfloat16 [16, 768, 16, 128], P('fsdp', 'seq'), may hold values from -6 to 6
- value_rows: bfloat16 [16, 768, 16, 128], P('fsdp', 'seq'), may hold values from -6 to 6
- gate_rows: bfloat16 [16, 768, 16, 128], P('fsdp', 'seq'), may hold values from -6 to 6
- out_weight: bfloat16 [2048, 2048], P('fsdp'), may hold values from -0.125 to 0.125
Outputs:
- block_out: bfloat16 [16, 768, 2048], P('fsdp', 'seq')
The draws below stay inside these ranges and needn't reach their ends.
All inputs are finite; a program needn't handle non-finite values.
Results may differ from the reference program's by a relative error of at most 0.006.
Values may be sent and summed in bfloat16 or wider, within the bound.
A program may use at most 64 MiB of HBM per device.

```python
import jax
import jax.numpy as jnp
from jax import lax

HEADS = 16
HEAD_SIZE = 128
BATCH = 16
TOKENS = 768
WIDTH = 2048


def block_scale(own_key, dims, shards, low, top_value):
    loudness, own = 1.0, jax.random.fold_in(own_key, 6)
    for axis_at, blocks in shards:
        steps = jnp.exp(jax.random.uniform(jax.random.fold_in(own, axis_at), (blocks,), jnp.float32, low / len(shards), top_value / len(shards)))
        loudness = loudness * jnp.repeat(steps, dims[axis_at] // blocks).reshape([-1 if axis == axis_at else 1 for axis in range(len(dims))])
    return loudness


def gaussian(rng, extent, deviation, reach, split=(), dtype=jnp.bfloat16):
    drawn = jax.random.normal(rng, extent, jnp.float32) * deviation
    if len(split) > 0:
        drawn = block_scale(rng, extent, split, -0.22, 0.18) * drawn
    return jnp.clip(drawn, min=-reach, max=reach).astype(dtype)


def setup_inputs(seed: int = 0) -> dict:
    keys = jax.random.split(jax.random.key(seed), 6)
    query_rows = gaussian(keys[0], (BATCH, TOKENS, HEADS, HEAD_SIZE), 1.0, 6.0, ((0, 8), (1, 4)))
    key_rows = gaussian(keys[1], (BATCH, TOKENS, HEADS, HEAD_SIZE), 1.0, 6.0, ((0, 8), (1, 4)))
    value_rows = gaussian(keys[2], (BATCH, TOKENS, HEADS, HEAD_SIZE), 1.0, 6.0, ((0, 8), (1, 4)))
    gate_rows = gaussian(keys[3], (BATCH, TOKENS, HEADS, HEAD_SIZE), 1.0, 6.0, ((0, 8), (1, 4)))
    out_weight = gaussian(keys[4], (WIDTH, WIDTH), WIDTH ** -0.5, 0.125, ((0, 8),))
    return dict(query_rows=query_rows, key_rows=key_rows, value_rows=value_rows, gate_rows=gate_rows, out_weight=out_weight)


def feature_map(values):
    wide = values.astype(jnp.float32)
    return (wide * wide + 0.1).astype(jnp.bfloat16)


def finish_heads(read, gate_rows, count):
    result = read * count ** 0.5
    result = result * jax.nn.sigmoid(gate_rows.astype(jnp.float32))
    return result.astype(jnp.bfloat16)


def read_state(features, state, mass):
    small = lax.optimization_barrier(state.astype(jnp.bfloat16))
    top = jnp.einsum("bthd,bhde->bthe", features.astype(jnp.float32), small.astype(jnp.float32))
    bottom = jnp.einsum("bthd,bhd->bth", features.astype(jnp.float32), mass, precision=lax.Precision.HIGHEST)
    return top / (bottom + 1e-3)[..., None]


def reference(query_rows, key_rows, value_rows, gate_rows, out_weight):
    query_feature, key_feature = lax.optimization_barrier((feature_map(query_rows), feature_map(key_rows)))
    state = jnp.einsum("bthd,bthe->bhde", key_feature.astype(jnp.float32), value_rows.astype(jnp.float32)) / TOKENS
    mass = jnp.sum(key_feature.astype(jnp.float32), axis=1) / TOKENS
    mixed = finish_heads(read_state(query_feature, state, mass), gate_rows, TOKENS).reshape(BATCH, TOKENS, WIDTH)
    mixed = lax.optimization_barrier(mixed)
    block_out = jnp.einsum("btw,wv->btv", mixed.astype(jnp.float32), out_weight.astype(jnp.float32)).astype(jnp.bfloat16)
    return block_out
```

```python
import functools
import math

import jax
import jax.numpy as jnp
from jax import lax
from jax.experimental import pallas as pl
from jax.experimental.pallas import tpu as pltpu
from jax.sharding import PartitionSpec as P

MESH = pl.DeviceIdType.MESH
CHUNK_HEADS = 2
HOP_LAG = 3
STAGE_EIGHTHS = 8
SECOND_EIGHTHS = 2
VMEM_MIB = 52
PIECES = 2
COLUMN_TILE = 512


def feature_map(wide):
    return (wide * wide + 0.1).astype(jnp.bfloat16)


def chip_grid(fsdp):
    chips = fsdp // 2
    along_x = max(size for size in range(1, math.isqrt(chips) + 1) if chips % size == 0)
    return chips // along_x, along_x


def kernel(
    fsdp,
    seq,
    q_hbm,
    k_hbm,
    v_hbm,
    g_hbm,
    w_hbm,
    *rest,
):
    results, rest = rest[: q_hbm.shape[0]], rest[q_hbm.shape[0] :]
    attend(fsdp, seq, q_hbm, k_hbm, v_hbm, g_hbm, w_hbm, results, *rest)


def attend(
    fsdp,
    seq,
    q_hbm,
    k_hbm,
    v_hbm,
    g_hbm,
    w_hbm,
    results,
    q_raw,
    k_raw,
    v_raw,
    g_raw,
    q_wide,
    k_wide,
    v_wide,
    g_wide,
    own,
    own_mass,
    came,
    gone,
    came_mass,
    gone_mass,
    weight,
    mixed,
    total,
    load_sem,
    state_send,
    state_recv,
    mass_send,
    mass_recv,
    ring_send,
    ring_recv,
    core_send,
    core_recv,
):
    batch, tokens, heads, size = q_raw.shape
    rows = w_hbm.shape[0]
    width = weight.shape[1]
    count = tokens * seq
    grid_y, grid_x = chip_grid(fsdp)
    group_heads = heads // (grid_x * grid_y)
    together = math.gcd(CHUNK_HEADS, group_heads)
    turns = heads // together
    group_turns = group_heads // together
    chunks = batch * turns
    places = sorted(
        ((i, j) for i in range(grid_x) for j in range(grid_y)), key=lambda place: (sum(place), place[1])
    )
    last_stage = grid_x + grid_y - 2

    f, z = lax.axis_index("fsdp"), lax.axis_index("seq")
    core, chip = lax.rem(f, 2), f // 2
    x, y = lax.rem(chip, grid_x), chip // grid_x

    def at(chip_y, chip_x, which):
        return (chip_y * grid_x + chip_x) * 2 + which

    right_x = at(y, lax.rem(x + 1, grid_x), core)
    right_y = at(lax.rem(y + 1, grid_y), x, core)
    other_core = at(y, x, 1 - core)

    loads = {}
    for number, (name, source, target) in enumerate(
        (("k", k_hbm, k_raw), ("v", v_hbm, v_raw), ("q", q_hbm, q_raw), ("g", g_hbm, g_raw))
    ):
        loads[name] = (source, target, number)

    def load(name, b):
        source, target, number = loads[name]
        return pltpu.make_async_copy(source.at[b], target.at[b], load_sem.at[number, b])

    own_rows = weight.at[pl.ds(pl.multiple_of(f * rows, rows), rows), :]
    load_weight = pltpu.make_async_copy(w_hbm, own_rows, load_sem.at[4, 0])
    load_weight.start()
    for b in range(batch):
        load("k", b).start()
        load("v", b).start()
    for b in range(batch):
        load("q", b).start()
        load("g", b).start()

    barrier = pltpu.get_barrier_semaphore()
    greeted = [{"fsdp": other_core}]
    if grid_x > 1:
        greeted.append({"fsdp": right_x})
    if grid_x > 2:
        greeted.append({"fsdp": at(y, lax.rem(x + grid_x - 1, grid_x), core)})
    if grid_y > 1:
        greeted.append({"fsdp": right_y})
    if grid_y > 2:
        greeted.append({"fsdp": at(lax.rem(y + grid_y - 1, grid_y), x, core)})
    for device in greeted:
        pl.semaphore_signal(barrier, inc=1, device_id=device, device_id_type=MESH)

    @pl.when(z > 0)
    def _():
        pl.semaphore_signal(barrier, inc=1, device_id={"seq": z - 1}, device_id_type=MESH)

    @pl.when(z < seq - 1)
    def _():
        pl.semaphore_signal(barrier, inc=1, device_id={"seq": z + 1}, device_id_type=MESH)

    ends = jnp.where(z > 0, 1, 0) + jnp.where(z < seq - 1, 1, 0)
    load_weight.wait()
    pl.semaphore_wait(barrier, len(greeted) + ends)

    piece_rows = rows // (2 * PIECES)

    def piece(place, color, part, which):
        i, j = place
        owner = at(lax.rem(y - j + grid_y, grid_y), lax.rem(x - i + grid_x, grid_x), which)
        start = owner * rows + (color * PIECES + part) * piece_rows
        return weight.at[pl.ds(pl.multiple_of(start, piece_rows), piece_rows), :]

    number_of = {place: number for number, place in enumerate(places)}

    def slot(place, color, part):
        return (number_of[place] * 2 + color) * PIECES + part

    def ring_copy(place, color, part, along):
        further = (place[0] + 1, place[1]) if along == "x" else (place[0], place[1] + 1)
        block, landing = piece(place, color, part, core), slot(further, color, part)
        return pltpu.make_async_remote_copy(
            src_ref=block,
            dst_ref=block,
            send_sem=ring_send.at[landing],
            recv_sem=ring_recv.at[landing],
            device_id={"fsdp": right_x if along == "x" else right_y},
            device_id_type=MESH,
        )

    def core_copy(place, color, part, which):
        block = piece(place, color, part, which)
        return pltpu.make_async_remote_copy(
            src_ref=block,
            dst_ref=block,
            send_sem=core_send.at[slot(place, color, part)],
            recv_sem=core_recv.at[slot(place, color, part)],
            device_id={"fsdp": other_core},
            device_id_type=MESH,
        )

    def onward(place, color):
        i, j = place
        ways = []
        if color == 0:
            if j == 0 and i < grid_x - 1:
                ways.append("x")
            if j < grid_y - 1:
                ways.append("y")
        else:
            if i == 0 and j < grid_y - 1:
                ways.append("y")
            if i < grid_x - 1:
                ways.append("x")
        return ways

    def came_along(place, color):
        i, j = place
        if color == 0:
            return ("y", (i, j - 1)) if j > 0 else ("x", (i - 1, j))
        return ("x", (i - 1, j)) if i > 0 else ("y", (i, j - 1))

    def stage(number, orders=(0, 1)):
        for order in orders:
            for part in range(PIECES):
                for place in places:
                    if sum(place) != number:
                        continue
                    for color in range(2):
                        if order == 0 and number > 0:
                            along, before = came_along(place, color)
                            block, landing = piece(place, color, part, core), slot(place, color, part)
                            pltpu.make_async_remote_copy(
                                src_ref=block,
                                dst_ref=block,
                                send_sem=ring_send.at[landing],
                                recv_sem=ring_recv.at[landing],
                                device_id={"fsdp": right_x},
                                device_id_type=MESH,
                            ).wait_recv()
                        ways = onward(place, color)
                        if order < len(ways):
                            ring_copy(place, color, part, ways[order]).start()
                        if order == 0:
                            core_copy(place, color, part, core).start()

    stage(0, (0,))

    leading = jnp.where(z < seq // 2, 0, 1)
    trailing = 1 - leading

    def has_in(d):
        return jnp.where(d == 0, z, seq - 1 - z) > 0

    def has_out(d):
        return jnp.where(d == 0, seq - 1 - z, z) > 0

    def state_copy(d, c):
        return pltpu.make_async_remote_copy(
            src_ref=gone.at[d, c],
            dst_ref=came.at[d, c],
            send_sem=state_send.at[d, c],
            recv_sem=state_recv.at[d, c],
            device_id={"seq": z + 1 - 2 * d},
            device_id_type=MESH,
        )

    def mass_copy(d, b):
        return pltpu.make_async_remote_copy(
            src_ref=gone_mass.at[d, b],
            dst_ref=came_mass.at[d, b],
            send_sem=mass_send.at[d, b],
            recv_sem=mass_recv.at[d, b],
            device_id={"seq": z + 1 - 2 * d},
            device_id_type=MESH,
        )

    def relay(d, c):
        b = c // turns

        @pl.when(lax.rem(c, turns) == 0)
        def _():
            @pl.when(has_in(d))
            def _():
                mass_copy(d, b).wait_recv()

            @pl.when(jnp.logical_not(has_in(d)))
            def _():
                came_mass[d, b] = jnp.zeros_like(came_mass[d, b])

            @pl.when(has_out(d))
            def _():
                gone_mass[d, b] = own_mass[b] + came_mass[d, b]
                mass_copy(d, b).start()

        @pl.when(has_in(d))
        def _():
            state_copy(d, c).wait_recv()

            @pl.when(has_out(d))
            def _():
                gone[d, c] = (own[c] + came[d, c].astype(jnp.float32)).astype(jnp.bfloat16)
                state_copy(d, c).start()

        @pl.when(jnp.logical_not(has_in(d)))
        def _():
            came[d, c] = jnp.zeros_like(came[d, c])

            @pl.when(has_out(d))
            def _():
                gone[d, c] = own[c].astype(jnp.bfloat16)
                state_copy(d, c).start()

    def group_of(o):
        i = j = 0
        for number, place in enumerate(places):
            i = jnp.where(o == number, place[0], i)
            j = jnp.where(o == number, place[1], j)
        return lax.rem(y - j + grid_y, grid_y) * grid_x + lax.rem(x - i + grid_x, grid_x)

    def head_of(c, n):
        order = lax.rem(c, turns) * together + n
        return group_of(order // group_heads) * group_heads + lax.rem(order, group_heads)

    step_tokens = 16

    def widen_kv(b):
        load("k", b).wait()
        load("v", b).wait()

        def body(n, mass):
            here = pl.ds(n * step_tokens, step_tokens)
            flat = pl.ds(pl.multiple_of(n * step_tokens * heads, step_tokens * heads), step_tokens * heads)
            feature = feature_map(k_raw[b, here].astype(jnp.float32)).astype(jnp.float32)
            k_wide[b, flat, :] = feature.reshape(step_tokens * heads, size)
            v_wide[b, flat, :] = v_raw[b, here].astype(jnp.float32).reshape(step_tokens * heads, size)
            return mass + jnp.sum(feature, axis=0)

        own_mass[b] = lax.fori_loop(0, tokens // step_tokens, body, jnp.zeros((heads, size), jnp.float32))

    def widen_qg(b):
        load("q", b).wait()
        load("g", b).wait()

        def body(n, carry):
            here = pl.ds(n * step_tokens, step_tokens)
            flat = pl.ds(pl.multiple_of(n * step_tokens * heads, step_tokens * heads), step_tokens * heads)
            q = q_raw[b, here].astype(jnp.float32)
            q_wide[b, flat, :] = (q * q + 0.1).reshape(step_tokens * heads, size)
            g = g_raw[b, here].astype(jnp.float32)
            g_wide[b, flat, :] = (count**0.5 / (1.0 + jnp.exp(-g))).reshape(step_tokens * heads, size)
            return carry

        lax.fori_loop(0, tokens // step_tokens, body, 0)

    def own_state(c, n):
        b, head = c // turns, head_of(c, n)
        feature = k_wide[b, pl.ds(head, tokens, stride=heads), :].astype(jnp.bfloat16)
        value = v_wide[b, pl.ds(head, tokens, stride=heads), :].astype(jnp.bfloat16)
        own[c, n] = lax.dot_general(
            value, feature, (((0,), (0,)), ((), ())), preferred_element_type=jnp.float32
        )

    def read(c, n):
        b, head = c // turns, head_of(c, n)
        state = own[c, n] + came[0, c, n].astype(jnp.float32) + came[1, c, n].astype(jnp.float32)
        one = pl.ds(head, 1)
        mass = own_mass[b, one] + came_mass[0, b, one] + came_mass[1, b, one]
        both = jnp.concatenate(
            [(state / count).astype(jnp.bfloat16), jnp.broadcast_to((mass / count).astype(jnp.bfloat16), state.shape)],
            axis=0,
        )
        feature = q_wide[b, pl.ds(head, tokens, stride=heads), :].astype(jnp.bfloat16)
        found = lax.dot_general(feature, both, (((1,), (1,)), ((), ())), preferred_element_type=jnp.float32)
        gate = g_wide[b, pl.ds(head, tokens, stride=heads), :]
        done = found[:, :size] / (found[:, size:] + 0.001) * gate
        columns = pl.ds(pl.multiple_of(head * size, size), size)
        mixed[pl.ds(pl.multiple_of(b * tokens, tokens), tokens), columns] = done.astype(jnp.bfloat16)

    def project(o):
        place = places[o]
        if sum(place) == last_stage and (o == 0 or sum(places[o - 1]) != last_stage):
            stage(last_stage) if last_stage > 0 else None
        for color in range(2):
            for part in range(PIECES):
                core_copy(place, color, part, 1 - core).wait_recv()
        deep = group_heads * size
        here = pl.ds(pl.multiple_of(group_of(o) * deep, deep), deep)

        def body(n, carry):
            columns = pl.ds(pl.multiple_of(n * COLUMN_TILE, COLUMN_TILE), COLUMN_TILE)
            term = jnp.dot(mixed[:, here], weight[here, columns], preferred_element_type=jnp.float32)
            if o > 0:
                term = total[:, columns] + term
            if o < len(places) - 1:
                total[:, columns] = term
            else:
                for b in range(batch):
                    results[b][:, columns] = term[b * tokens : (b + 1) * tokens].astype(jnp.bfloat16)
            return carry

        lax.fori_loop(0, width // COLUMN_TILE, body, 0)

    nearer = jnp.minimum(z, seq - 1 - z)
    lead_lag = nearer * HOP_LAG
    trail_lag = (seq - 1 - nearer) * HOP_LAG

    def step(k, carry):
        late = k - trail_lag

        @pl.when(jnp.logical_and(k - lead_lag >= 0, k - lead_lag < chunks))
        def _():
            relay(leading, k - lead_lag)

        @pl.when(jnp.logical_and(late >= 0, late < chunks))
        def _():
            relay(trailing, late)

        @pl.when(k == SECOND_EIGHTHS * chunks // 8)
        def _():
            stage(0, (1,))

        for number in range(1, last_stage):
            @pl.when(k == number * STAGE_EIGHTHS * chunks // (8 * (last_stage - 1)))
            def _():
                stage(number)

        later = k + 1

        @pl.when(jnp.logical_and(later < chunks, lax.rem(later, turns) == 0))
        def _():
            widen_kv(later // turns)

        @pl.when(later < chunks)
        def _():
            for n in range(together):
                own_state(later, n)

        @pl.when(jnp.logical_and(late + 1 >= 0, jnp.logical_and(late + 1 < chunks, lax.rem(late + 1, turns) == 0)))
        def _():
            widen_qg((late + 1) // turns)

        @pl.when(jnp.logical_and(late >= 0, late < chunks))
        def _():
            for n in range(together):
                read(late, n)

        for o in range(len(places)):
            @pl.when(late == chunks - turns + group_turns * (o + 1) - 1)
            def _():
                project(o)

        return carry

    widen_kv(0)
    for n in range(together):
        own_state(0, n)
    lax.fori_loop(0, chunks + (seq - 1) * HOP_LAG, step, 0)

    for place in places:
        for color in range(2):
            for part in range(PIECES):
                core_copy(place, color, part, core).wait_send()
                for along in onward(place, color):
                    ring_copy(place, color, part, along).wait_send()
    for d in range(2):

        @pl.when(has_out(d))
        def _():
            for b in range(batch):
                mass_copy(d, b).wait_send()

            def body(c, carry):
                state_copy(d, c).wait_send()
                return carry

            lax.fori_loop(0, chunks, body, 0)


def store(*refs):
    *parts, out, sem = refs
    copies = [pltpu.make_async_copy(part, out.at[b], sem.at[b]) for b, part in enumerate(parts)]
    for copy in copies:
        copy.start()
    for copy in copies:
        copy.wait()


def local(fsdp, seq, query_rows, key_rows, value_rows, gate_rows, out_weight):
    batch, tokens, heads, size = query_rows.shape
    rows, width = out_weight.shape
    grid_y, grid_x = chip_grid(fsdp)
    slots = grid_x * grid_y * 2 * PIECES
    together = math.gcd(CHUNK_HEADS, heads // (grid_x * grid_y))
    chunks = batch * heads // together
    raw = pltpu.VMEM(query_rows.shape, jnp.bfloat16)
    wide = pltpu.VMEM((batch, tokens * heads, size), jnp.float32)
    dma = pltpu.SemaphoreType.DMA
    parts = pl.pallas_call(
        functools.partial(kernel, fsdp, seq),
        out_shape=[jax.ShapeDtypeStruct((tokens, width), jnp.bfloat16)] * batch,
        in_specs=[pl.BlockSpec(memory_space=pl.ANY)] * 5,
        out_specs=[pl.BlockSpec(memory_space=pltpu.VMEM)] * batch,
        scratch_shapes=[
            raw,
            raw,
            raw,
            raw,
            wide,
            wide,
            wide,
            wide,
            pltpu.VMEM((chunks, together, size, size), jnp.float32),
            pltpu.VMEM((batch, heads, size), jnp.float32),
            pltpu.VMEM((2, chunks, together, size, size), jnp.bfloat16),
            pltpu.VMEM((2, chunks, together, size, size), jnp.bfloat16),
            pltpu.VMEM((2, batch, heads, size), jnp.float32),
            pltpu.VMEM((2, batch, heads, size), jnp.float32),
            pltpu.VMEM((rows * fsdp, width), jnp.bfloat16),
            pltpu.VMEM((batch * tokens, heads * size), jnp.bfloat16),
            pltpu.VMEM((batch * tokens, width), jnp.float32),
            dma((5, batch)),
            dma((2, chunks)),
            dma((2, chunks)),
            dma((2, batch)),
            dma((2, batch)),
            dma((slots,)),
            dma((slots,)),
            dma((slots,)),
            dma((slots,)),
        ],
        compiler_params=pltpu.CompilerParams(
            collective_id=0, has_side_effects=True, vmem_limit_bytes=VMEM_MIB * 1024 * 1024
        ),
        name="attend",
    )(query_rows, key_rows, value_rows, gate_rows, out_weight)
    return pl.pallas_call(
        store,
        out_shape=jax.ShapeDtypeStruct((batch, tokens, width), jnp.bfloat16),
        in_specs=[pl.BlockSpec(memory_space=pl.ANY)] * batch,
        out_specs=pl.BlockSpec(memory_space=pl.ANY),
        scratch_shapes=[dma((batch,))],
        compiler_params=pltpu.CompilerParams(vmem_limit_bytes=8 * 1024 * 1024),
        name="store",
    )(*parts)


def solution(mesh):
    row_spec = P("fsdp", "seq", None, None)
    return jax.shard_map(
        functools.partial(local, mesh.shape["fsdp"], mesh.shape["seq"]),
        mesh=mesh,
        in_specs=(row_spec, row_spec, row_spec, row_spec, P("fsdp", None)),
        out_specs=P("fsdp", "seq", None),
        check_vma=False,
    )
```

```python
import functools
import math

import jax
import jax.numpy as jnp
from jax import lax
from jax.experimental import pallas as pl
from jax.experimental.pallas import tpu as pltpu
from jax.sharding import PartitionSpec as P

MESH = pl.DeviceIdType.MESH
CHUNK_HEADS = 2
HOP_LAG = 3
STAGE_EIGHTHS = 8
SECOND_EIGHTHS = 2
VMEM_MIB = 52
PIECES = 2
COLUMN_TILE = 1024


def feature_map(wide):
    return (wide * wide + 0.1).astype(jnp.bfloat16)


def chip_grid(fsdp):
    chips = fsdp // 2
    along_x = max(size for size in range(1, math.isqrt(chips) + 1) if chips % size == 0)
    return chips // along_x, along_x


def kernel(
    fsdp,
    seq,
    q_hbm,
    k_hbm,
    v_hbm,
    g_hbm,
    w_hbm,
    *rest,
):
    results, rest = rest[: q_hbm.shape[0]], rest[q_hbm.shape[0] :]
    attend(fsdp, seq, q_hbm, k_hbm, v_hbm, g_hbm, w_hbm, results, *rest)


def attend(
    fsdp,
    seq,
    q_hbm,
    k_hbm,
    v_hbm,
    g_hbm,
    w_hbm,
    results,
    q_raw,
    k_raw,
    v_raw,
    g_raw,
    q_wide,
    k_wide,
    v_wide,
    g_wide,
    own,
    own_mass,
    came,
    gone,
    came_mass,
    gone_mass,
    weight,
    mixed,
    total,
    load_sem,
    state_send,
    state_recv,
    mass_send,
    mass_recv,
    ring_send,
    ring_recv,
    core_send,
    core_recv,
):
    batch, tokens, heads, size = q_raw.shape
    rows = w_hbm.shape[0]
    width = weight.shape[1]
    count = tokens * seq
    grid_y, grid_x = chip_grid(fsdp)
    group_heads = heads // (grid_x * grid_y)
    together = math.gcd(CHUNK_HEADS, group_heads)
    turns = heads // together
    group_turns = group_heads // together
    chunks = batch * turns
    places = sorted(
        ((i, j) for i in range(grid_x) for j in range(grid_y)), key=lambda place: (sum(place), place[1])
    )
    last_stage = grid_x + grid_y - 2

    f, z = lax.axis_index("fsdp"), lax.axis_index("seq")
    core, chip = lax.rem(f, 2), f // 2
    x, y = lax.rem(chip, grid_x), chip // grid_x

    def at(chip_y, chip_x, which):
        return (chip_y * grid_x + chip_x) * 2 + which

    right_x = at(y, lax.rem(x + 1, grid_x), core)
    right_y = at(lax.rem(y + 1, grid_y), x, core)
    other_core = at(y, x, 1 - core)

    loads = {}
    for number, (name, source, target) in enumerate(
        (("k", k_hbm, k_raw), ("v", v_hbm, v_raw), ("q", q_hbm, q_raw), ("g", g_hbm, g_raw))
    ):
        loads[name] = (source, target, number)

    def load(name, b):
        source, target, number = loads[name]
        return pltpu.make_async_copy(source.at[b], target.at[b], load_sem.at[number, b])

    own_rows = weight.at[pl.ds(pl.multiple_of(f * rows, rows), rows), :]
    load_weight = pltpu.make_async_copy(w_hbm, own_rows, load_sem.at[4, 0])
    load_weight.start()
    for b in range(batch):
        load("k", b).start()
        load("v", b).start()
    for b in range(batch):
        load("q", b).start()
        load("g", b).start()

    barrier = pltpu.get_barrier_semaphore()
    greeted = [{"fsdp": other_core}]
    if grid_x > 1:
        greeted.append({"fsdp": right_x})
    if grid_x > 2:
        greeted.append({"fsdp": at(y, lax.rem(x + grid_x - 1, grid_x), core)})
    if grid_y > 1:
        greeted.append({"fsdp": right_y})
    if grid_y > 2:
        greeted.append({"fsdp": at(lax.rem(y + grid_y - 1, grid_y), x, core)})
    for device in greeted:
        pl.semaphore_signal(barrier, inc=1, device_id=device, device_id_type=MESH)

    @pl.when(z > 0)
    def _():
        pl.semaphore_signal(barrier, inc=1, device_id={"seq": z - 1}, device_id_type=MESH)

    @pl.when(z < seq - 1)
    def _():
        pl.semaphore_signal(barrier, inc=1, device_id={"seq": z + 1}, device_id_type=MESH)

    ends = jnp.where(z > 0, 1, 0) + jnp.where(z < seq - 1, 1, 0)
    load_weight.wait()
    pl.semaphore_wait(barrier, len(greeted) + ends)

    piece_rows = rows // (2 * PIECES)

    def piece(place, color, part, which):
        i, j = place
        owner = at(lax.rem(y - j + grid_y, grid_y), lax.rem(x - i + grid_x, grid_x), which)
        start = owner * rows + (color * PIECES + part) * piece_rows
        return weight.at[pl.ds(pl.multiple_of(start, piece_rows), piece_rows), :]

    number_of = {place: number for number, place in enumerate(places)}

    def slot(place, color, part):
        return (number_of[place] * 2 + color) * PIECES + part

    def ring_copy(place, color, part, along):
        further = (place[0] + 1, place[1]) if along == "x" else (place[0], place[1] + 1)
        block, landing = piece(place, color, part, core), slot(further, color, part)
        return pltpu.make_async_remote_copy(
            src_ref=block,
            dst_ref=block,
            send_sem=ring_send.at[landing],
            recv_sem=ring_recv.at[landing],
            device_id={"fsdp": right_x if along == "x" else right_y},
            device_id_type=MESH,
        )

    def core_copy(place, color, part, which):
        block = piece(place, color, part, which)
        return pltpu.make_async_remote_copy(
            src_ref=block,
            dst_ref=block,
            send_sem=core_send.at[slot(place, color, part)],
            recv_sem=core_recv.at[slot(place, color, part)],
            device_id={"fsdp": other_core},
            device_id_type=MESH,
        )

    def onward(place, color):
        i, j = place
        ways = []
        if color == 0:
            if j == 0 and i < grid_x - 1:
                ways.append("x")
            if j < grid_y - 1:
                ways.append("y")
        else:
            if i == 0 and j < grid_y - 1:
                ways.append("y")
            if i < grid_x - 1:
                ways.append("x")
        return ways

    def came_along(place, color):
        i, j = place
        if color == 0:
            return ("y", (i, j - 1)) if j > 0 else ("x", (i - 1, j))
        return ("x", (i - 1, j)) if i > 0 else ("y", (i, j - 1))

    def stage(number, orders=(0, 1)):
        for order in orders:
            for part in range(PIECES):
                for place in places:
                    if sum(place) != number:
                        continue
                    for color in range(2):
                        if order == 0 and number > 0:
                            along, before = came_along(place, color)
                            block, landing = piece(place, color, part, core), slot(place, color, part)
                            pltpu.make_async_remote_copy(
                                src_ref=block,
                                dst_ref=block,
                                send_sem=ring_send.at[landing],
                                recv_sem=ring_recv.at[landing],
                                device_id={"fsdp": right_x},
                                device_id_type=MESH,
                            ).wait_recv()
                        ways = onward(place, color)
                        if order < len(ways):
                            ring_copy(place, color, part, ways[order]).start()
                        if order == 0:
                            core_copy(place, color, part, core).start()

    stage(0, (0,))

    leading = jnp.where(z < seq // 2, 0, 1)
    trailing = 1 - leading

    def has_in(d):
        return jnp.where(d == 0, z, seq - 1 - z) > 0

    def has_out(d):
        return jnp.where(d == 0, seq - 1 - z, z) > 0

    def state_copy(d, c):
        return pltpu.make_async_remote_copy(
            src_ref=gone.at[d, c],
            dst_ref=came.at[d, c],
            send_sem=state_send.at[d, c],
            recv_sem=state_recv.at[d, c],
            device_id={"seq": z + 1 - 2 * d},
            device_id_type=MESH,
        )

    def mass_copy(d, b):
        return pltpu.make_async_remote_copy(
            src_ref=gone_mass.at[d, b],
            dst_ref=came_mass.at[d, b],
            send_sem=mass_send.at[d, b],
            recv_sem=mass_recv.at[d, b],
            device_id={"seq": z + 1 - 2 * d},
            device_id_type=MESH,
        )

    def relay(d, c):
        b = c // turns

        @pl.when(lax.rem(c, turns) == 0)
        def _():
            @pl.when(has_in(d))
            def _():
                mass_copy(d, b).wait_recv()

            @pl.when(jnp.logical_not(has_in(d)))
            def _():
                came_mass[d, b] = jnp.zeros_like(came_mass[d, b])

            @pl.when(has_out(d))
            def _():
                gone_mass[d, b] = own_mass[b] + came_mass[d, b]
                mass_copy(d, b).start()

        @pl.when(has_in(d))
        def _():
            state_copy(d, c).wait_recv()

            @pl.when(has_out(d))
            def _():
                gone[d, c] = (own[c] + came[d, c].astype(jnp.float32)).astype(jnp.bfloat16)
                state_copy(d, c).start()

        @pl.when(jnp.logical_not(has_in(d)))
        def _():
            came[d, c] = jnp.zeros_like(came[d, c])

            @pl.when(has_out(d))
            def _():
                gone[d, c] = own[c].astype(jnp.bfloat16)
                state_copy(d, c).start()

    def group_of(o):
        i = j = 0
        for number, place in enumerate(places):
            i = jnp.where(o == number, place[0], i)
            j = jnp.where(o == number, place[1], j)
        return lax.rem(y - j + grid_y, grid_y) * grid_x + lax.rem(x - i + grid_x, grid_x)

    def head_of(c, n):
        order = lax.rem(c, turns) * together + n
        return group_of(order // group_heads) * group_heads + lax.rem(order, group_heads)

    step_tokens = 16

    def widen_kv(b):
        load("k", b).wait()
        load("v", b).wait()

        def body(n, mass):
            here = pl.ds(n * step_tokens, step_tokens)
            flat = pl.ds(pl.multiple_of(n * step_tokens * heads, step_tokens * heads), step_tokens * heads)
            feature = feature_map(k_raw[b, here].astype(jnp.float32)).astype(jnp.float32)
            k_wide[b, flat, :] = feature.reshape(step_tokens * heads, size)
            v_wide[b, flat, :] = v_raw[b, here].astype(jnp.float32).reshape(step_tokens * heads, size)
            return mass + jnp.sum(feature, axis=0)

        own_mass[b] = lax.fori_loop(0, tokens // step_tokens, body, jnp.zeros((heads, size), jnp.float32))

    def widen_qg(b):
        load("q", b).wait()
        load("g", b).wait()

        def body(n, carry):
            here = pl.ds(n * step_tokens, step_tokens)
            flat = pl.ds(pl.multiple_of(n * step_tokens * heads, step_tokens * heads), step_tokens * heads)
            q = q_raw[b, here].astype(jnp.float32)
            q_wide[b, flat, :] = (q * q + 0.1).reshape(step_tokens * heads, size)
            g = g_raw[b, here].astype(jnp.float32)
            g_wide[b, flat, :] = (count**0.5 / (1.0 + jnp.exp(-g))).reshape(step_tokens * heads, size)
            return carry

        lax.fori_loop(0, tokens // step_tokens, body, 0)

    def own_state(c, n):
        b, head = c // turns, head_of(c, n)
        feature = k_wide[b, pl.ds(head, tokens, stride=heads), :].astype(jnp.bfloat16)
        value = v_wide[b, pl.ds(head, tokens, stride=heads), :].astype(jnp.bfloat16)
        own[c, n] = lax.dot_general(
            value, feature, (((0,), (0,)), ((), ())), preferred_element_type=jnp.float32
        )

    def read(c, n):
        b, head = c // turns, head_of(c, n)
        state = own[c, n] + came[0, c, n].astype(jnp.float32) + came[1, c, n].astype(jnp.float32)
        one = pl.ds(head, 1)
        mass = own_mass[b, one] + came_mass[0, b, one] + came_mass[1, b, one]
        both = jnp.concatenate(
            [(state / count).astype(jnp.bfloat16), jnp.broadcast_to((mass / count).astype(jnp.bfloat16), state.shape)],
            axis=0,
        )
        feature = q_wide[b, pl.ds(head, tokens, stride=heads), :].astype(jnp.bfloat16)
        found = lax.dot_general(feature, both, (((1,), (1,)), ((), ())), preferred_element_type=jnp.float32)
        gate = g_wide[b, pl.ds(head, tokens, stride=heads), :]
        done = found[:, :size] / (found[:, size:] + 0.001) * gate
        columns = pl.ds(pl.multiple_of(head * size, size), size)
        mixed[pl.ds(pl.multiple_of(b * tokens, tokens), tokens), columns] = done.astype(jnp.bfloat16)

    def project(o):
        place = places[o]
        if sum(place) == last_stage and (o == 0 or sum(places[o - 1]) != last_stage):
            stage(last_stage) if last_stage > 0 else None
        for color in range(2):
            for part in range(PIECES):
                core_copy(place, color, part, 1 - core).wait_recv()
        deep = group_heads * size
        here = pl.ds(pl.multiple_of(group_of(o) * deep, deep), deep)

        def body(n, carry):
            columns = pl.ds(pl.multiple_of(n * COLUMN_TILE, COLUMN_TILE), COLUMN_TILE)
            term = jnp.dot(mixed[:, here], weight[here, columns], preferred_element_type=jnp.float32)
            if o > 0:
                term = total[:, columns] + term
            if o < len(places) - 1:
                total[:, columns] = term
            else:
                for b in range(batch):
                    results[b][:, columns] = term[b * tokens : (b + 1) * tokens].astype(jnp.bfloat16)
            return carry

        lax.fori_loop(0, width // COLUMN_TILE, body, 0)

    nearer = jnp.minimum(z, seq - 1 - z)
    lead_lag = nearer * HOP_LAG
    trail_lag = (seq - 1 - nearer) * HOP_LAG

    def step(k, carry):
        late = k - trail_lag

        @pl.when(jnp.logical_and(k - lead_lag >= 0, k - lead_lag < chunks))
        def _():
            relay(leading, k - lead_lag)

        @pl.when(jnp.logical_and(late >= 0, late < chunks))
        def _():
            relay(trailing, late)

        @pl.when(k == SECOND_EIGHTHS * chunks // 8)
        def _():
            stage(0, (1,))

        for number in range(1, last_stage):
            @pl.when(k == number * STAGE_EIGHTHS * chunks // (8 * (last_stage - 1)))
            def _():
                stage(number)

        later = k + 1

        @pl.when(jnp.logical_and(later < chunks, lax.rem(later, turns) == 0))
        def _():
            widen_kv(later // turns)

        @pl.when(later < chunks)
        def _():
            for n in range(together):
                own_state(later, n)

        @pl.when(jnp.logical_and(late + 1 >= 0, jnp.logical_and(late + 1 < chunks, lax.rem(late + 1, turns) == 0)))
        def _():
            widen_qg((late + 1) // turns)

        @pl.when(jnp.logical_and(late >= 0, late < chunks))
        def _():
            for n in range(together):
                read(late, n)

        for o in range(len(places)):
            @pl.when(late == chunks - turns + group_turns * (o + 1) - 1)
            def _():
                project(o)

        return carry

    widen_kv(0)
    for n in range(together):
        own_state(0, n)
    lax.fori_loop(0, chunks + (seq - 1) * HOP_LAG, step, 0)

    for place in places:
        for color in range(2):
            for part in range(PIECES):
                core_copy(place, color, part, core).wait_send()
                for along in onward(place, color):
                    ring_copy(place, color, part, along).wait_send()
    for d in range(2):

        @pl.when(has_out(d))
        def _():
            for b in range(batch):
                mass_copy(d, b).wait_send()

            def body(c, carry):
                state_copy(d, c).wait_send()
                return carry

            lax.fori_loop(0, chunks, body, 0)


def store(*refs):
    *parts, out, sem = refs
    copies = [pltpu.make_async_copy(part, out.at[b], sem.at[b]) for b, part in enumerate(parts)]
    for copy in copies:
        copy.start()
    for copy in copies:
        copy.wait()


def local(fsdp, seq, query_rows, key_rows, value_rows, gate_rows, out_weight):
    batch, tokens, heads, size = query_rows.shape
    rows, width = out_weight.shape
    grid_y, grid_x = chip_grid(fsdp)
    slots = grid_x * grid_y * 2 * PIECES
    together = math.gcd(CHUNK_HEADS, heads // (grid_x * grid_y))
    chunks = batch * heads // together
    raw = pltpu.VMEM(query_rows.shape, jnp.bfloat16)
    wide = pltpu.VMEM((batch, tokens * heads, size), jnp.float32)
    dma = pltpu.SemaphoreType.DMA
    parts = pl.pallas_call(
        functools.partial(kernel, fsdp, seq),
        out_shape=[jax.ShapeDtypeStruct((tokens, width), jnp.bfloat16)] * batch,
        in_specs=[pl.BlockSpec(memory_space=pl.ANY)] * 5,
        out_specs=[pl.BlockSpec(memory_space=pltpu.VMEM)] * batch,
        scratch_shapes=[
            raw,
            raw,
            raw,
            raw,
            wide,
            wide,
            wide,
            wide,
            pltpu.VMEM((chunks, together, size, size), jnp.float32),
            pltpu.VMEM((batch, heads, size), jnp.float32),
            pltpu.VMEM((2, chunks, together, size, size), jnp.bfloat16),
            pltpu.VMEM((2, chunks, together, size, size), jnp.bfloat16),
            pltpu.VMEM((2, batch, heads, size), jnp.float32),
            pltpu.VMEM((2, batch, heads, size), jnp.float32),
            pltpu.VMEM((rows * fsdp, width), jnp.bfloat16),
            pltpu.VMEM((batch * tokens, heads * size), jnp.bfloat16),
            pltpu.VMEM((batch * tokens, width), jnp.float32),
            dma((5, batch)),
            dma((2, chunks)),
            dma((2, chunks)),
            dma((2, batch)),
            dma((2, batch)),
            dma((slots,)),
            dma((slots,)),
            dma((slots,)),
            dma((slots,)),
        ],
        compiler_params=pltpu.CompilerParams(
            collective_id=0, has_side_effects=True, vmem_limit_bytes=VMEM_MIB * 1024 * 1024
        ),
        name="attend",
    )(query_rows, key_rows, value_rows, gate_rows, out_weight)
    return pl.pallas_call(
        store,
        out_shape=jax.ShapeDtypeStruct((batch, tokens, width), jnp.bfloat16),
        in_specs=[pl.BlockSpec(memory_space=pl.ANY)] * batch,
        out_specs=pl.BlockSpec(memory_space=pl.ANY),
        scratch_shapes=[dma((batch,))],
        compiler_params=pltpu.CompilerParams(vmem_limit_bytes=8 * 1024 * 1024),
        name="store",
    )(*parts)


def solution(mesh):
    row_spec = P("fsdp", "seq", None, None)
    return jax.shard_map(
        functools.partial(local, mesh.shape["fsdp"], mesh.shape["seq"]),
        mesh=mesh,
        in_specs=(row_spec, row_spec, row_spec, row_spec, P("fsdp", None)),
        out_specs=P("fsdp", "seq", None),
        check_vma=False,
    )
```

```python
import functools
import math

import jax
import jax.numpy as jnp
from jax import lax
from jax.experimental import pallas as pl
from jax.experimental.pallas import tpu as pltpu
from jax.sharding import PartitionSpec as P

MESH = pl.DeviceIdType.MESH
CHUNK_HEADS = 2
HOP_LAG = 3
STAGE_EIGHTHS = 8
SECOND_EIGHTHS = 2
VMEM_MIB = 52
PIECES = 2
COLUMN_TILE = 1024


def feature_map(wide):
    return (wide * wide + 0.1).astype(jnp.bfloat16)


def chip_grid(fsdp):
    chips = fsdp // 2
    along_x = max(size for size in range(1, math.isqrt(chips) + 1) if chips % size == 0)
    return chips // along_x, along_x


def kernel(
    fsdp,
    seq,
    q_hbm,
    k_hbm,
    v_hbm,
    g_hbm,
    w_hbm,
    *rest,
):
    results, rest = rest[: q_hbm.shape[0]], rest[q_hbm.shape[0] :]
    attend(fsdp, seq, q_hbm, k_hbm, v_hbm, g_hbm, w_hbm, results, *rest)


def attend(
    fsdp,
    seq,
    q_hbm,
    k_hbm,
    v_hbm,
    g_hbm,
    w_hbm,
    results,
    q_raw,
    k_raw,
    v_raw,
    g_raw,
    q_wide,
    k_wide,
    v_wide,
    g_wide,
    own,
    own_mass,
    came,
    gone,
    came_mass,
    gone_mass,
    weight,
    mixed,
    total,
    load_sem,
    state_send,
    state_recv,
    mass_send,
    mass_recv,
    ring_send,
    ring_recv,
    core_send,
    core_recv,
):
    batch, tokens, heads, size = q_raw.shape
    rows = w_hbm.shape[0]
    width = weight.shape[1]
    count = tokens * seq
    grid_y, grid_x = chip_grid(fsdp)
    group_heads = heads // (grid_x * grid_y)
    together = math.gcd(CHUNK_HEADS, group_heads)
    turns = heads // together
    group_turns = group_heads // together
    chunks = batch * turns
    places = sorted(
        ((i, j) for i in range(grid_x) for j in range(grid_y)), key=lambda place: (sum(place), place[1])
    )
    last_stage = grid_x + grid_y - 2

    f, z = lax.axis_index("fsdp"), lax.axis_index("seq")
    core, chip = lax.rem(f, 2), f // 2
    x, y = lax.rem(chip, grid_x), chip // grid_x

    def at(chip_y, chip_x, which):
        return (chip_y * grid_x + chip_x) * 2 + which

    right_x = at(y, lax.rem(x + 1, grid_x), core)
    right_y = at(lax.rem(y + 1, grid_y), x, core)
    other_core = at(y, x, 1 - core)

    loads = {}
    for number, (name, source, target) in enumerate(
        (("k", k_hbm, k_raw), ("v", v_hbm, v_raw), ("q", q_hbm, q_raw), ("g", g_hbm, g_raw))
    ):
        loads[name] = (source, target, number)

    def load(name, b):
        source, target, number = loads[name]
        return pltpu.make_async_copy(source.at[b], target.at[b], load_sem.at[number, b])

    own_rows = weight.at[pl.ds(pl.multiple_of(f * rows, rows), rows), :]
    load_weight = pltpu.make_async_copy(w_hbm, own_rows, load_sem.at[4, 0])
    load_weight.start()
    for b in range(batch):
        load("k", b).start()
        load("v", b).start()
    for b in range(batch):
        load("q", b).start()
        load("g", b).start()

    barrier = pltpu.get_barrier_semaphore()
    greeted = [{"fsdp": other_core}]
    if grid_x > 1:
        greeted.append({"fsdp": right_x})
    if grid_x > 2:
        greeted.append({"fsdp": at(y, lax.rem(x + grid_x - 1, grid_x), core)})
    if grid_y > 1:
        greeted.append({"fsdp": right_y})
    if grid_y > 2:
        greeted.append({"fsdp": at(lax.rem(y + grid_y - 1, grid_y), x, core)})
    for device in greeted:
        pl.semaphore_signal(barrier, inc=1, device_id=device, device_id_type=MESH)

    @pl.when(z > 0)
    def _():
        pl.semaphore_signal(barrier, inc=1, device_id={"seq": z - 1}, device_id_type=MESH)

    @pl.when(z < seq - 1)
    def _():
        pl.semaphore_signal(barrier, inc=1, device_id={"seq": z + 1}, device_id_type=MESH)

    ends = jnp.where(z > 0, 1, 0) + jnp.where(z < seq - 1, 1, 0)
    load_weight.wait()
    pl.semaphore_wait(barrier, len(greeted) + ends)

    piece_rows = rows // (2 * PIECES)

    def piece(place, color, part, which):
        i, j = place
        owner = at(lax.rem(y - j + grid_y, grid_y), lax.rem(x - i + grid_x, grid_x), which)
        start = owner * rows + (color * PIECES + part) * piece_rows
        return weight.at[pl.ds(pl.multiple_of(start, piece_rows), piece_rows), :]

    number_of = {place: number for number, place in enumerate(places)}

    def slot(place, color, part):
        return (number_of[place] * 2 + color) * PIECES + part

    def ring_copy(place, color, part, along):
        further = (place[0] + 1, place[1]) if along == "x" else (place[0], place[1] + 1)
        block, landing = piece(place, color, part, core), slot(further, color, part)
        return pltpu.make_async_remote_copy(
            src_ref=block,
            dst_ref=block,
            send_sem=ring_send.at[landing],
            recv_sem=ring_recv.at[landing],
            device_id={"fsdp": right_x if along == "x" else right_y},
            device_id_type=MESH,
        )

    def core_copy(place, color, part, which):
        block = piece(place, color, part, which)
        return pltpu.make_async_remote_copy(
            src_ref=block,
            dst_ref=block,
            send_sem=core_send.at[slot(place, color, part)],
            recv_sem=core_recv.at[slot(place, color, part)],
            device_id={"fsdp": other_core},
            device_id_type=MESH,
        )

    def onward(place, color):
        i, j = place
        ways = []
        if color == 0:
            if j == 0 and i < grid_x - 1:
                ways.append("x")
            if j < grid_y - 1:
                ways.append("y")
        else:
            if i == 0 and j < grid_y - 1:
                ways.append("y")
            if i < grid_x - 1:
                ways.append("x")
        return ways

    def came_along(place, color):
        i, j = place
        if color == 0:
            return ("y", (i, j - 1)) if j > 0 else ("x", (i - 1, j))
        return ("x", (i - 1, j)) if i > 0 else ("y", (i, j - 1))

    def stage(number, orders=(0, 1)):
        for order in orders:
            for part in range(PIECES):
                for place in places:
                    if sum(place) != number:
                        continue
                    for color in range(2):
                        if order == 0 and number > 0:
                            along, before = came_along(place, color)
                            block, landing = piece(place, color, part, core), slot(place, color, part)
                            pltpu.make_async_remote_copy(
                                src_ref=block,
                                dst_ref=block,
                                send_sem=ring_send.at[landing],
                                recv_sem=ring_recv.at[landing],
                                device_id={"fsdp": right_x},
                                device_id_type=MESH,
                            ).wait_recv()
                        ways = onward(place, color)
                        if order < len(ways):
                            ring_copy(place, color, part, ways[order]).start()
                        if order == 0:
                            core_copy(place, color, part, core).start()

    stage(0, (0,))

    leading = jnp.where(z < seq // 2, 0, 1)
    trailing = 1 - leading

    def has_in(d):
        return jnp.where(d == 0, z, seq - 1 - z) > 0

    def has_out(d):
        return jnp.where(d == 0, seq - 1 - z, z) > 0

    def state_copy(d, c):
        return pltpu.make_async_remote_copy(
            src_ref=gone.at[d, c],
            dst_ref=came.at[d, c],
            send_sem=state_send.at[d, c],
            recv_sem=state_recv.at[d, c],
            device_id={"seq": z + 1 - 2 * d},
            device_id_type=MESH,
        )

    def mass_copy(d, b):
        return pltpu.make_async_remote_copy(
            src_ref=gone_mass.at[d, b],
            dst_ref=came_mass.at[d, b],
            send_sem=mass_send.at[d, b],
            recv_sem=mass_recv.at[d, b],
            device_id={"seq": z + 1 - 2 * d},
            device_id_type=MESH,
        )

    def relay(d, c):
        b = c // turns

        @pl.when(lax.rem(c, turns) == 0)
        def _():
            @pl.when(has_in(d))
            def _():
                mass_copy(d, b).wait_recv()

            @pl.when(jnp.logical_not(has_in(d)))
            def _():
                came_mass[d, b] = jnp.zeros_like(came_mass[d, b])

            @pl.when(has_out(d))
            def _():
                gone_mass[d, b] = own_mass[b] + came_mass[d, b]
                mass_copy(d, b).start()

        @pl.when(has_in(d))
        def _():
            state_copy(d, c).wait_recv()

            @pl.when(has_out(d))
            def _():
                gone[d, c] = (own[c] + came[d, c].astype(jnp.float32)).astype(jnp.bfloat16)
                state_copy(d, c).start()

        @pl.when(jnp.logical_not(has_in(d)))
        def _():
            came[d, c] = jnp.zeros_like(came[d, c])

            @pl.when(has_out(d))
            def _():
                gone[d, c] = own[c].astype(jnp.bfloat16)
                state_copy(d, c).start()

    def group_of(o):
        i = j = 0
        for number, place in enumerate(places):
            i = jnp.where(o == number, place[0], i)
            j = jnp.where(o == number, place[1], j)
        return lax.rem(y - j + grid_y, grid_y) * grid_x + lax.rem(x - i + grid_x, grid_x)

    def head_of(c, n):
        order = lax.rem(c, turns) * together + n
        return group_of(order // group_heads) * group_heads + lax.rem(order, group_heads)

    step_tokens = 16

    def widen_kv(b):
        load("k", b).wait()
        load("v", b).wait()

        def body(n, mass):
            here = pl.ds(n * step_tokens, step_tokens)
            flat = pl.ds(pl.multiple_of(n * step_tokens * heads, step_tokens * heads), step_tokens * heads)
            feature = feature_map(k_raw[b, here].astype(jnp.float32)).astype(jnp.float32)
            k_wide[b, flat, :] = feature.reshape(step_tokens * heads, size)
            v_wide[b, flat, :] = v_raw[b, here].astype(jnp.float32).reshape(step_tokens * heads, size)
            return mass + jnp.sum(feature, axis=0)

        own_mass[b] = lax.fori_loop(0, tokens // step_tokens, body, jnp.zeros((heads, size), jnp.float32))

    def widen_qg(b):
        load("q", b).wait()
        load("g", b).wait()

        def body(n, carry):
            here = pl.ds(n * step_tokens, step_tokens)
            flat = pl.ds(pl.multiple_of(n * step_tokens * heads, step_tokens * heads), step_tokens * heads)
            q = q_raw[b, here].astype(jnp.float32)
            q_wide[b, flat, :] = (q * q + 0.1).reshape(step_tokens * heads, size)
            g = g_raw[b, here].astype(jnp.float32)
            g_wide[b, flat, :] = (count**0.5 / (1.0 + jnp.exp(-g))).reshape(step_tokens * heads, size)
            return carry

        lax.fori_loop(0, tokens // step_tokens, body, 0)

    def own_state(c, n):
        b, head = c // turns, head_of(c, n)
        feature = k_wide[b, pl.ds(head, tokens, stride=heads), :].astype(jnp.bfloat16)
        value = v_wide[b, pl.ds(head, tokens, stride=heads), :].astype(jnp.bfloat16)
        own[c, n] = lax.dot_general(
            value, feature, (((0,), (0,)), ((), ())), preferred_element_type=jnp.float32
        )

    def read(c, n):
        b, head = c // turns, head_of(c, n)
        state = own[c, n] + came[0, c, n].astype(jnp.float32) + came[1, c, n].astype(jnp.float32)
        one = pl.ds(head, 1)
        mass = own_mass[b, one] + came_mass[0, b, one] + came_mass[1, b, one]
        both = jnp.concatenate(
            [(state / count).astype(jnp.bfloat16), jnp.broadcast_to((mass / count).astype(jnp.bfloat16), state.shape)],
            axis=0,
        )
        feature = q_wide[b, pl.ds(head, tokens, stride=heads), :].astype(jnp.bfloat16)
        found = lax.dot_general(feature, both, (((1,), (1,)), ((), ())), preferred_element_type=jnp.float32)
        gate = g_wide[b, pl.ds(head, tokens, stride=heads), :]
        done = found[:, :size] / (found[:, size:] + 0.001) * gate
        columns = pl.ds(pl.multiple_of(head * size, size), size)
        mixed[pl.ds(pl.multiple_of(b * tokens, tokens), tokens), columns] = done.astype(jnp.bfloat16)

    def project(o):
        place = places[o]
        if sum(place) == last_stage and (o == 0 or sum(places[o - 1]) != last_stage):
            stage(last_stage) if last_stage > 0 else None
        last = o == len(places) - 1
        if last and rows % 128 == 0 and o > 0:
            project_part(o, group_of(o) * 2 * rows + core * rows, rows, False)
            arrived(place)
            project_part(o, group_of(o) * 2 * rows + (1 - core) * rows, rows, True)
        else:
            arrived(place)
            project_part(o, group_of(o) * 2 * rows, 2 * rows, last)

    def arrived(place):
        for color in range(2):
            for part in range(PIECES):
                core_copy(place, color, part, 1 - core).wait_recv()

    def project_part(o, start, deep, last):
        here = pl.ds(pl.multiple_of(start, deep), deep)

        def body(n, carry):
            columns = pl.ds(pl.multiple_of(n * COLUMN_TILE, COLUMN_TILE), COLUMN_TILE)
            term = jnp.dot(mixed[:, here], weight[here, columns], preferred_element_type=jnp.float32)
            if o > 0:
                term = total[:, columns] + term
            if not last:
                total[:, columns] = term
            else:
                for b in range(batch):
                    results[b][:, columns] = term[b * tokens : (b + 1) * tokens].astype(jnp.bfloat16)
            return carry

        lax.fori_loop(0, width // COLUMN_TILE, body, 0)

    nearer = jnp.minimum(z, seq - 1 - z)
    lead_lag = nearer * HOP_LAG
    trail_lag = (seq - 1 - nearer) * HOP_LAG

    def step(k, carry):
        late = k - trail_lag

        @pl.when(jnp.logical_and(k - lead_lag >= 0, k - lead_lag < chunks))
        def _():
            relay(leading, k - lead_lag)

        @pl.when(jnp.logical_and(late >= 0, late < chunks))
        def _():
            relay(trailing, late)

        @pl.when(k == SECOND_EIGHTHS * chunks // 8)
        def _():
            stage(0, (1,))

        for number in range(1, last_stage):
            @pl.when(k == number * STAGE_EIGHTHS * chunks // (8 * (last_stage - 1)))
            def _():
                stage(number)

        later = k + 1

        @pl.when(jnp.logical_and(later < chunks, lax.rem(later, turns) == 0))
        def _():
            widen_kv(later // turns)

        @pl.when(later < chunks)
        def _():
            for n in range(together):
                own_state(later, n)

        @pl.when(jnp.logical_and(late + 1 >= 0, jnp.logical_and(late + 1 < chunks, lax.rem(late + 1, turns) == 0)))
        def _():
            widen_qg((late + 1) // turns)

        @pl.when(jnp.logical_and(late >= 0, late < chunks))
        def _():
            for n in range(together):
                read(late, n)

        for o in range(len(places)):
            @pl.when(late == chunks - turns + group_turns * (o + 1) - 1)
            def _():
                project(o)

        return carry

    widen_kv(0)
    for n in range(together):
        own_state(0, n)
    lax.fori_loop(0, chunks + (seq - 1) * HOP_LAG, step, 0)

    for place in places:
        for color in range(2):
            for part in range(PIECES):
                core_copy(place, color, part, core).wait_send()
                for along in onward(place, color):
                    ring_copy(place, color, part, along).wait_send()
    for d in range(2):

        @pl.when(has_out(d))
        def _():
            for b in range(batch):
                mass_copy(d, b).wait_send()

            def body(c, carry):
                state_copy(d, c).wait_send()
                return carry

            lax.fori_loop(0, chunks, body, 0)


def store(*refs):
    *parts, out, sem = refs
    copies = [pltpu.make_async_copy(part, out.at[b], sem.at[b]) for b, part in enumerate(parts)]
    for copy in copies:
        copy.start()
    for copy in copies:
        copy.wait()


def local(fsdp, seq, query_rows, key_rows, value_rows, gate_rows, out_weight):
    batch, tokens, heads, size = query_rows.shape
    rows, width = out_weight.shape
    grid_y, grid_x = chip_grid(fsdp)
    slots = grid_x * grid_y * 2 * PIECES
    together = math.gcd(CHUNK_HEADS, heads // (grid_x * grid_y))
    chunks = batch * heads // together
    raw = pltpu.VMEM(query_rows.shape, jnp.bfloat16)
    wide = pltpu.VMEM((batch, tokens * heads, size), jnp.float32)
    dma = pltpu.SemaphoreType.DMA
    parts = pl.pallas_call(
        functools.partial(kernel, fsdp, seq),
        out_shape=[jax.ShapeDtypeStruct((tokens, width), jnp.bfloat16)] * batch,
        in_specs=[pl.BlockSpec(memory_space=pl.ANY)] * 5,
        out_specs=[pl.BlockSpec(memory_space=pltpu.VMEM)] * batch,
        scratch_shapes=[
            raw,
            raw,
            raw,
            raw,
            wide,
            wide,
            wide,
            wide,
            pltpu.VMEM((chunks, together, size, size), jnp.float32),
            pltpu.VMEM((batch, heads, size), jnp.float32),
            pltpu.VMEM((2, chunks, together, size, size), jnp.bfloat16),
            pltpu.VMEM((2, chunks, together, size, size), jnp.bfloat16),
            pltpu.VMEM((2, batch, heads, size), jnp.float32),
            pltpu.VMEM((2, batch, heads, size), jnp.float32),
            pltpu.VMEM((rows * fsdp, width), jnp.bfloat16),
            pltpu.VMEM((batch * tokens, heads * size), jnp.bfloat16),
            pltpu.VMEM((batch * tokens, width), jnp.float32),
            dma((5, batch)),
            dma((2, chunks)),
            dma((2, chunks)),
            dma((2, batch)),
            dma((2, batch)),
            dma((slots,)),
            dma((slots,)),
            dma((slots,)),
            dma((slots,)),
        ],
        compiler_params=pltpu.CompilerParams(
            collective_id=0, has_side_effects=True, vmem_limit_bytes=VMEM_MIB * 1024 * 1024
        ),
        name="attend",
    )(query_rows, key_rows, value_rows, gate_rows, out_weight)
    return pl.pallas_call(
        store,
        out_shape=jax.ShapeDtypeStruct((batch, tokens, width), jnp.bfloat16),
        in_specs=[pl.BlockSpec(memory_space=pl.ANY)] * batch,
        out_specs=pl.BlockSpec(memory_space=pl.ANY),
        scratch_shapes=[dma((batch,))],
        compiler_params=pltpu.CompilerParams(vmem_limit_bytes=8 * 1024 * 1024),
        name="store",
    )(*parts)


def solution(mesh):
    row_spec = P("fsdp", "seq", None, None)
    return jax.shard_map(
        functools.partial(local, mesh.shape["fsdp"], mesh.shape["seq"]),
        mesh=mesh,
        in_specs=(row_spec, row_spec, row_spec, row_spec, P("fsdp", None)),
        out_specs=P("fsdp", "seq", None),
        check_vma=False,
    )
```

```python
import functools
import math

import jax
import jax.numpy as jnp
from jax import lax
from jax.experimental import pallas as pl
from jax.experimental.pallas import tpu as pltpu
from jax.sharding import PartitionSpec as P

MESH = pl.DeviceIdType.MESH
CHUNK_HEADS = 2
HOP_LAG = 3
STAGE_SIXTEENTHS = 16
SECOND_SIXTEENTHS = 5
VMEM_MIB = 52
PIECES = 2
COLUMN_TILE = 2048


def feature_map(wide):
    return (wide * wide + 0.1).astype(jnp.bfloat16)


def chip_grid(fsdp):
    chips = fsdp // 2
    along_x = max(size for size in range(1, math.isqrt(chips) + 1) if chips % size == 0)
    return chips // along_x, along_x


def kernel(
    fsdp,
    seq,
    q_hbm,
    k_hbm,
    v_hbm,
    g_hbm,
    w_hbm,
    *rest,
):
    results, rest = rest[: q_hbm.shape[0]], rest[q_hbm.shape[0] :]
    attend(fsdp, seq, q_hbm, k_hbm, v_hbm, g_hbm, w_hbm, results, *rest)


def attend(
    fsdp,
    seq,
    q_hbm,
    k_hbm,
    v_hbm,
    g_hbm,
    w_hbm,
    results,
    q_raw,
    k_raw,
    v_raw,
    g_raw,
    q_wide,
    k_wide,
    v_wide,
    g_wide,
    own,
    own_mass,
    came,
    gone,
    came_mass,
    gone_mass,
    weight,
    mixed,
    total,
    load_sem,
    state_send,
    state_recv,
    mass_send,
    mass_recv,
    ring_send,
    ring_recv,
    core_send,
    core_recv,
):
    batch, tokens, heads, size = q_raw.shape
    rows = w_hbm.shape[0]
    width = weight.shape[1]
    count = tokens * seq
    grid_y, grid_x = chip_grid(fsdp)
    group_heads = heads // (grid_x * grid_y)
    together = math.gcd(CHUNK_HEADS, group_heads)
    turns = heads // together
    group_turns = group_heads // together
    chunks = batch * turns
    places = sorted(
        ((i, j) for i in range(grid_x) for j in range(grid_y)), key=lambda place: (sum(place), place[1])
    )
    last_stage = grid_x + grid_y - 2

    f, z = lax.axis_index("fsdp"), lax.axis_index("seq")
    core, chip = lax.rem(f, 2), f // 2
    x, y = lax.rem(chip, grid_x), chip // grid_x

    def at(chip_y, chip_x, which):
        return (chip_y * grid_x + chip_x) * 2 + which

    right_x = at(y, lax.rem(x + 1, grid_x), core)
    right_y = at(lax.rem(y + 1, grid_y), x, core)
    other_core = at(y, x, 1 - core)

    loads = {}
    for number, (name, source, target) in enumerate(
        (("k", k_hbm, k_raw), ("v", v_hbm, v_raw), ("q", q_hbm, q_raw), ("g", g_hbm, g_raw))
    ):
        loads[name] = (source, target, number)

    def load(name, b):
        source, target, number = loads[name]
        return pltpu.make_async_copy(source.at[b], target.at[b], load_sem.at[number, b])

    own_rows = weight.at[pl.ds(pl.multiple_of(f * rows, rows), rows), :]
    load_weight = pltpu.make_async_copy(w_hbm, own_rows, load_sem.at[4, 0])
    load_weight.start()
    for b in range(batch):
        load("k", b).start()
        load("v", b).start()

    barrier = pltpu.get_barrier_semaphore()
    greeted = [{"fsdp": other_core}]
    if grid_x > 1:
        greeted.append({"fsdp": right_x})
    if grid_x > 2:
        greeted.append({"fsdp": at(y, lax.rem(x + grid_x - 1, grid_x), core)})
    if grid_y > 1:
        greeted.append({"fsdp": right_y})
    if grid_y > 2:
        greeted.append({"fsdp": at(lax.rem(y + grid_y - 1, grid_y), x, core)})
    for device in greeted:
        pl.semaphore_signal(barrier, inc=1, device_id=device, device_id_type=MESH)

    @pl.when(z > 0)
    def _():
        pl.semaphore_signal(barrier, inc=1, device_id={"seq": z - 1}, device_id_type=MESH)

    @pl.when(z < seq - 1)
    def _():
        pl.semaphore_signal(barrier, inc=1, device_id={"seq": z + 1}, device_id_type=MESH)

    ends = jnp.where(z > 0, 1, 0) + jnp.where(z < seq - 1, 1, 0)
    load_weight.wait()
    pl.semaphore_wait(barrier, len(greeted) + ends)

    piece_rows = rows // (2 * PIECES)

    def piece(place, color, part, which):
        i, j = place
        owner = at(lax.rem(y - j + grid_y, grid_y), lax.rem(x - i + grid_x, grid_x), which)
        start = owner * rows + (color * PIECES + part) * piece_rows
        return weight.at[pl.ds(pl.multiple_of(start, piece_rows), piece_rows), :]

    number_of = {place: number for number, place in enumerate(places)}

    def slot(place, color, part):
        return (number_of[place] * 2 + color) * PIECES + part

    def ring_copy(place, color, part, along):
        further = (place[0] + 1, place[1]) if along == "x" else (place[0], place[1] + 1)
        block, landing = piece(place, color, part, core), slot(further, color, part)
        return pltpu.make_async_remote_copy(
            src_ref=block,
            dst_ref=block,
            send_sem=ring_send.at[landing],
            recv_sem=ring_recv.at[landing],
            device_id={"fsdp": right_x if along == "x" else right_y},
            device_id_type=MESH,
        )

    def core_copy(place, color, part, which):
        block = piece(place, color, part, which)
        return pltpu.make_async_remote_copy(
            src_ref=block,
            dst_ref=block,
            send_sem=core_send.at[slot(place, color, part)],
            recv_sem=core_recv.at[slot(place, color, part)],
            device_id={"fsdp": other_core},
            device_id_type=MESH,
        )

    def onward(place, color):
        i, j = place
        ways = []
        if color == 0:
            if j == 0 and i < grid_x - 1:
                ways.append("x")
            if j < grid_y - 1:
                ways.append("y")
        else:
            if i == 0 and j < grid_y - 1:
                ways.append("y")
            if i < grid_x - 1:
                ways.append("x")
        return ways

    def came_along(place, color):
        i, j = place
        if color == 0:
            return ("y", (i, j - 1)) if j > 0 else ("x", (i - 1, j))
        return ("x", (i - 1, j)) if i > 0 else ("y", (i, j - 1))

    def stage(number, orders=(0, 1)):
        for order in orders:
            for part in range(PIECES):
                for place in places:
                    if sum(place) != number:
                        continue
                    for color in range(2):
                        if order == 0 and number > 0:
                            along, before = came_along(place, color)
                            block, landing = piece(place, color, part, core), slot(place, color, part)
                            pltpu.make_async_remote_copy(
                                src_ref=block,
                                dst_ref=block,
                                send_sem=ring_send.at[landing],
                                recv_sem=ring_recv.at[landing],
                                device_id={"fsdp": right_x},
                                device_id_type=MESH,
                            ).wait_recv()
                        ways = onward(place, color)
                        if order < len(ways):
                            ring_copy(place, color, part, ways[order]).start()
                        if order == 0:
                            core_copy(place, color, part, core).start()

    stage(0, (0,))
    for b in range(batch):
        load("q", b).start()
        load("g", b).start()

    leading = jnp.where(z < seq // 2, 0, 1)
    trailing = 1 - leading

    def has_in(d):
        return jnp.where(d == 0, z, seq - 1 - z) > 0

    def has_out(d):
        return jnp.where(d == 0, seq - 1 - z, z) > 0

    def state_copy(d, c):
        return pltpu.make_async_remote_copy(
            src_ref=gone.at[d, c],
            dst_ref=came.at[d, c],
            send_sem=state_send.at[d, c],
            recv_sem=state_recv.at[d, c],
            device_id={"seq": z + 1 - 2 * d},
            device_id_type=MESH,
        )

    def mass_copy(d, b):
        return pltpu.make_async_remote_copy(
            src_ref=gone_mass.at[d, b],
            dst_ref=came_mass.at[d, b],
            send_sem=mass_send.at[d, b],
            recv_sem=mass_recv.at[d, b],
            device_id={"seq": z + 1 - 2 * d},
            device_id_type=MESH,
        )

    def relay(d, c):
        b = c // turns

        @pl.when(lax.rem(c, turns) == 0)
        def _():
            @pl.when(has_in(d))
            def _():
                mass_copy(d, b).wait_recv()

            @pl.when(jnp.logical_not(has_in(d)))
            def _():
                came_mass[d, b] = jnp.zeros_like(came_mass[d, b])

            @pl.when(has_out(d))
            def _():
                gone_mass[d, b] = own_mass[b] + came_mass[d, b]
                mass_copy(d, b).start()

        @pl.when(has_in(d))
        def _():
            state_copy(d, c).wait_recv()

            @pl.when(has_out(d))
            def _():
                gone[d, c] = (own[c] + came[d, c].astype(jnp.float32)).astype(jnp.bfloat16)
                state_copy(d, c).start()

        @pl.when(jnp.logical_not(has_in(d)))
        def _():
            came[d, c] = jnp.zeros_like(came[d, c])

            @pl.when(has_out(d))
            def _():
                gone[d, c] = own[c].astype(jnp.bfloat16)
                state_copy(d, c).start()

    def group_of(o):
        i = j = 0
        for number, place in enumerate(places):
            i = jnp.where(o == number, place[0], i)
            j = jnp.where(o == number, place[1], j)
        return lax.rem(y - j + grid_y, grid_y) * grid_x + lax.rem(x - i + grid_x, grid_x)

    def head_of(c, n):
        order = lax.rem(c, turns) * together + n
        return group_of(order // group_heads) * group_heads + lax.rem(order, group_heads)

    step_tokens = 16

    def widen_kv(b):
        load("k", b).wait()
        load("v", b).wait()

        def body(n, mass):
            here = pl.ds(n * step_tokens, step_tokens)
            flat = pl.ds(pl.multiple_of(n * step_tokens * heads, step_tokens * heads), step_tokens * heads)
            feature = feature_map(k_raw[b, here].astype(jnp.float32)).astype(jnp.float32)
            k_wide[b, flat, :] = feature.reshape(step_tokens * heads, size)
            v_wide[b, flat, :] = v_raw[b, here].astype(jnp.float32).reshape(step_tokens * heads, size)
            return mass + jnp.sum(feature, axis=0)

        own_mass[b] = lax.fori_loop(0, tokens // step_tokens, body, jnp.zeros((heads, size), jnp.float32))

    def widen_qg(b):
        load("q", b).wait()
        load("g", b).wait()

        def body(n, carry):
            here = pl.ds(n * step_tokens, step_tokens)
            flat = pl.ds(pl.multiple_of(n * step_tokens * heads, step_tokens * heads), step_tokens * heads)
            q = q_raw[b, here].astype(jnp.float32)
            q_wide[b, flat, :] = (q * q + 0.1).reshape(step_tokens * heads, size)
            g = g_raw[b, here].astype(jnp.float32)
            g_wide[b, flat, :] = (count**0.5 / (1.0 + jnp.exp(-g))).reshape(step_tokens * heads, size)
            return carry

        lax.fori_loop(0, tokens // step_tokens, body, 0)

    def own_state(c, n):
        b, head = c // turns, head_of(c, n)
        feature = k_wide[b, pl.ds(head, tokens, stride=heads), :].astype(jnp.bfloat16)
        value = v_wide[b, pl.ds(head, tokens, stride=heads), :].astype(jnp.bfloat16)
        own[c, n] = lax.dot_general(
            value, feature, (((0,), (0,)), ((), ())), preferred_element_type=jnp.float32
        )

    def read(c, n):
        b, head = c // turns, head_of(c, n)
        state = own[c, n] + came[0, c, n].astype(jnp.float32) + came[1, c, n].astype(jnp.float32)
        one = pl.ds(head, 1)
        mass = own_mass[b, one] + came_mass[0, b, one] + came_mass[1, b, one]
        both = jnp.concatenate(
            [(state / count).astype(jnp.bfloat16), jnp.broadcast_to((mass / count).astype(jnp.bfloat16), state.shape)],
            axis=0,
        )
        feature = q_wide[b, pl.ds(head, tokens, stride=heads), :].astype(jnp.bfloat16)
        found = lax.dot_general(feature, both, (((1,), (1,)), ((), ())), preferred_element_type=jnp.float32)
        gate = g_wide[b, pl.ds(head, tokens, stride=heads), :]
        done = found[:, :size] / (found[:, size:] + 0.001) * gate
        columns = pl.ds(pl.multiple_of(head * size, size), size)
        mixed[pl.ds(pl.multiple_of(b * tokens, tokens), tokens), columns] = done.astype(jnp.bfloat16)

    def project(o):
        place = places[o]
        if sum(place) == last_stage and (o == 0 or sum(places[o - 1]) != last_stage):
            stage(last_stage) if last_stage > 0 else None
        last = o == len(places) - 1
        if last and rows % 128 == 0 and o > 0:
            project_part(o, group_of(o) * 2 * rows + core * rows, rows, False)
            arrived(place)
            project_part(o, group_of(o) * 2 * rows + (1 - core) * rows, rows, True)
        else:
            arrived(place)
            project_part(o, group_of(o) * 2 * rows, 2 * rows, last)

    def arrived(place):
        for color in range(2):
            for part in range(PIECES):
                core_copy(place, color, part, 1 - core).wait_recv()

    def project_part(o, start, deep, last):
        here = pl.ds(pl.multiple_of(start, deep), deep)

        def body(n, carry):
            columns = pl.ds(pl.multiple_of(n * COLUMN_TILE, COLUMN_TILE), COLUMN_TILE)
            term = jnp.dot(mixed[:, here], weight[here, columns], preferred_element_type=jnp.float32)
            if o > 0:
                term = total[:, columns] + term
            if not last:
                total[:, columns] = term
            else:
                for b in range(batch):
                    results[b][:, columns] = term[b * tokens : (b + 1) * tokens].astype(jnp.bfloat16)
            return carry

        lax.fori_loop(0, width // COLUMN_TILE, body, 0)

    nearer = jnp.minimum(z, seq - 1 - z)
    lead_lag = nearer * HOP_LAG
    trail_lag = (seq - 1 - nearer) * HOP_LAG

    def step(k, carry):
        late = k - trail_lag

        @pl.when(jnp.logical_and(k - lead_lag >= 0, k - lead_lag < chunks))
        def _():
            relay(leading, k - lead_lag)

        @pl.when(jnp.logical_and(late >= 0, late < chunks))
        def _():
            relay(trailing, late)

        @pl.when(k == SECOND_SIXTEENTHS * chunks // 16)
        def _():
            stage(0, (1,))

        for number in range(1, last_stage):
            @pl.when(k == number * STAGE_SIXTEENTHS * chunks // (16 * (last_stage - 1)))
            def _():
                stage(number)

        later = k + 1

        @pl.when(jnp.logical_and(later < chunks, lax.rem(later, turns) == 0))
        def _():
            widen_kv(later // turns)

        @pl.when(later < chunks)
        def _():
            for n in range(together):
                own_state(later, n)

        @pl.when(jnp.logical_and(late + 1 >= 0, jnp.logical_and(late + 1 < chunks, lax.rem(late + 1, turns) == 0)))
        def _():
            widen_qg((late + 1) // turns)

        @pl.when(jnp.logical_and(late >= 0, late < chunks))
        def _():
            for n in range(together):
                read(late, n)

        for o in range(len(places)):
            @pl.when(late == chunks - turns + group_turns * (o + 1) - 1)
            def _():
                project(o)

        return carry

    widen_kv(0)
    for n in range(together):
        own_state(0, n)
    lax.fori_loop(0, chunks + (seq - 1) * HOP_LAG, step, 0)

    for place in places:
        for color in range(2):
            for part in range(PIECES):
                core_copy(place, color, part, core).wait_send()
                for along in onward(place, color):
                    ring_copy(place, color, part, along).wait_send()
    for d in range(2):

        @pl.when(has_out(d))
        def _():
            for b in range(batch):
                mass_copy(d, b).wait_send()

            def body(c, carry):
                state_copy(d, c).wait_send()
                return carry

            lax.fori_loop(0, chunks, body, 0)


def store(*refs):
    *parts, out, sem = refs
    copies = [pltpu.make_async_copy(part, out.at[b], sem.at[b]) for b, part in enumerate(parts)]
    for copy in copies:
        copy.start()
    for copy in copies:
        copy.wait()


def local(fsdp, seq, query_rows, key_rows, value_rows, gate_rows, out_weight):
    batch, tokens, heads, size = query_rows.shape
    rows, width = out_weight.shape
    grid_y, grid_x = chip_grid(fsdp)
    slots = grid_x * grid_y * 2 * PIECES
    together = math.gcd(CHUNK_HEADS, heads // (grid_x * grid_y))
    chunks = batch * heads // together
    raw = pltpu.VMEM(query_rows.shape, jnp.bfloat16)
    wide = pltpu.VMEM((batch, tokens * heads, size), jnp.float32)
    dma = pltpu.SemaphoreType.DMA
    parts = pl.pallas_call(
        functools.partial(kernel, fsdp, seq),
        out_shape=[jax.ShapeDtypeStruct((tokens, width), jnp.bfloat16)] * batch,
        in_specs=[pl.BlockSpec(memory_space=pl.ANY)] * 5,
        out_specs=[pl.BlockSpec(memory_space=pltpu.VMEM)] * batch,
        scratch_shapes=[
            raw,
            raw,
            raw,
            raw,
            wide,
            wide,
            wide,
            wide,
            pltpu.VMEM((chunks, together, size, size), jnp.float32),
            pltpu.VMEM((batch, heads, size), jnp.float32),
            pltpu.VMEM((2, chunks, together, size, size), jnp.bfloat16),
            pltpu.VMEM((2, chunks, together, size, size), jnp.bfloat16),
            pltpu.VMEM((2, batch, heads, size), jnp.float32),
            pltpu.VMEM((2, batch, heads, size), jnp.float32),
            pltpu.VMEM((rows * fsdp, width), jnp.bfloat16),
            pltpu.VMEM((batch * tokens, heads * size), jnp.bfloat16),
            pltpu.VMEM((batch * tokens, width), jnp.float32),
            dma((5, batch)),
            dma((2, chunks)),
            dma((2, chunks)),
            dma((2, batch)),
            dma((2, batch)),
            dma((slots,)),
            dma((slots,)),
            dma((slots,)),
            dma((slots,)),
        ],
        compiler_params=pltpu.CompilerParams(
            collective_id=0, has_side_effects=True, vmem_limit_bytes=VMEM_MIB * 1024 * 1024
        ),
        name="attend",
    )(query_rows, key_rows, value_rows, gate_rows, out_weight)
    return pl.pallas_call(
        store,
        out_shape=jax.ShapeDtypeStruct((batch, tokens, width), jnp.bfloat16),
        in_specs=[pl.BlockSpec(memory_space=pl.ANY)] * batch,
        out_specs=pl.BlockSpec(memory_space=pl.ANY),
        scratch_shapes=[dma((batch,))],
        compiler_params=pltpu.CompilerParams(vmem_limit_bytes=8 * 1024 * 1024),
        name="store",
    )(*parts)


def solution(mesh):
    row_spec = P("fsdp", "seq", None, None)
    return jax.shard_map(
        functools.partial(local, mesh.shape["fsdp"], mesh.shape["seq"]),
        mesh=mesh,
        in_specs=(row_spec, row_spec, row_spec, row_spec, P("fsdp", None)),
        out_specs=P("fsdp", "seq", None),
        check_vma=False,
    )
```

```python
import functools
import math

import jax
import jax.numpy as jnp
from jax import lax
from jax.experimental import pallas as pl
from jax.experimental.pallas import tpu as pltpu
from jax.sharding import PartitionSpec as P

MESH = pl.DeviceIdType.MESH
CHUNK_HEADS = 2
HOP_LAG = 3
STAGE_SIXTEENTHS = 16
SECOND_SIXTEENTHS = 5
VMEM_MIB = 52
PIECES = 2
COLUMN_TILE = 2048


def feature_map(wide):
    return (wide * wide + 0.1).astype(jnp.bfloat16)


def chip_grid(fsdp):
    chips = fsdp // 2
    along_x = max(size for size in range(1, math.isqrt(chips) + 1) if chips % size == 0)
    return chips // along_x, along_x


def kernel(
    fsdp,
    seq,
    q_hbm,
    k_hbm,
    v_hbm,
    g_hbm,
    w_hbm,
    *rest,
):
    results, rest = rest[: q_hbm.shape[0]], rest[q_hbm.shape[0] :]
    attend(fsdp, seq, q_hbm, k_hbm, v_hbm, g_hbm, w_hbm, results, *rest)


def attend(
    fsdp,
    seq,
    q_hbm,
    k_hbm,
    v_hbm,
    g_hbm,
    w_hbm,
    results,
    q_raw,
    k_raw,
    v_raw,
    g_raw,
    q_wide,
    k_wide,
    v_wide,
    g_wide,
    own,
    own_mass,
    came,
    gone,
    came_mass,
    gone_mass,
    weight,
    mixed,
    total,
    load_sem,
    state_send,
    state_recv,
    mass_send,
    mass_recv,
    ring_send,
    ring_recv,
    core_send,
    core_recv,
):
    batch, tokens, heads, size = q_raw.shape
    rows = w_hbm.shape[0]
    width = weight.shape[1]
    count = tokens * seq
    grid_y, grid_x = chip_grid(fsdp)
    group_heads = heads // (grid_x * grid_y)
    together = math.gcd(CHUNK_HEADS, group_heads)
    turns = heads // together
    group_turns = group_heads // together
    chunks = batch * turns
    places = sorted(
        ((i, j) for i in range(grid_x) for j in range(grid_y)), key=lambda place: (sum(place), place[1])
    )
    last_stage = grid_x + grid_y - 2

    f, z = lax.axis_index("fsdp"), lax.axis_index("seq")
    core, chip = lax.rem(f, 2), f // 2
    x, y = lax.rem(chip, grid_x), chip // grid_x

    def at(chip_y, chip_x, which):
        return (chip_y * grid_x + chip_x) * 2 + which

    right_x = at(y, lax.rem(x + 1, grid_x), core)
    right_y = at(lax.rem(y + 1, grid_y), x, core)
    other_core = at(y, x, 1 - core)

    loads = {}
    for number, (name, source, target) in enumerate(
        (("k", k_hbm, k_raw), ("v", v_hbm, v_raw), ("q", q_hbm, q_raw), ("g", g_hbm, g_raw))
    ):
        loads[name] = (source, target, number)

    def load(name, b):
        source, target, number = loads[name]
        return pltpu.make_async_copy(source.at[b], target.at[b], load_sem.at[number, b])

    own_rows = weight.at[pl.ds(pl.multiple_of(f * rows, rows), rows), :]
    load_weight = pltpu.make_async_copy(w_hbm, own_rows, load_sem.at[4, 0])
    load_weight.start()
    for b in range(batch):
        load("k", b).start()
        load("v", b).start()

    barrier = pltpu.get_barrier_semaphore()
    greeted = [{"fsdp": other_core}]
    if grid_x > 1:
        greeted.append({"fsdp": right_x})
    if grid_x > 2:
        greeted.append({"fsdp": at(y, lax.rem(x + grid_x - 1, grid_x), core)})
    if grid_y > 1:
        greeted.append({"fsdp": right_y})
    if grid_y > 2:
        greeted.append({"fsdp": at(lax.rem(y + grid_y - 1, grid_y), x, core)})
    for device in greeted:
        pl.semaphore_signal(barrier, inc=1, device_id=device, device_id_type=MESH)

    @pl.when(z > 0)
    def _():
        pl.semaphore_signal(barrier, inc=1, device_id={"seq": z - 1}, device_id_type=MESH)

    @pl.when(z < seq - 1)
    def _():
        pl.semaphore_signal(barrier, inc=1, device_id={"seq": z + 1}, device_id_type=MESH)

    ends = jnp.where(z > 0, 1, 0) + jnp.where(z < seq - 1, 1, 0)
    load_weight.wait()
    pl.semaphore_wait(barrier, len(greeted) + ends)

    piece_rows = rows // (2 * PIECES)

    def piece(place, color, part, which):
        i, j = place
        owner = at(lax.rem(y - j + grid_y, grid_y), lax.rem(x - i + grid_x, grid_x), which)
        start = owner * rows + (color * PIECES + part) * piece_rows
        return weight.at[pl.ds(pl.multiple_of(start, piece_rows), piece_rows), :]

    number_of = {place: number for number, place in enumerate(places)}

    def slot(place, color, part):
        return (number_of[place] * 2 + color) * PIECES + part

    def ring_copy(place, color, part, along):
        further = (place[0] + 1, place[1]) if along == "x" else (place[0], place[1] + 1)
        block, landing = piece(place, color, part, core), slot(further, color, part)
        return pltpu.make_async_remote_copy(
            src_ref=block,
            dst_ref=block,
            send_sem=ring_send.at[landing],
            recv_sem=ring_recv.at[landing],
            device_id={"fsdp": right_x if along == "x" else right_y},
            device_id_type=MESH,
        )

    def core_copy(place, color, part, which):
        block = piece(place, color, part, which)
        return pltpu.make_async_remote_copy(
            src_ref=block,
            dst_ref=block,
            send_sem=core_send.at[slot(place, color, part)],
            recv_sem=core_recv.at[slot(place, color, part)],
            device_id={"fsdp": other_core},
            device_id_type=MESH,
        )

    def onward(place, color):
        i, j = place
        ways = []
        if color == 0:
            if j == 0 and i < grid_x - 1:
                ways.append("x")
            if j < grid_y - 1:
                ways.append("y")
        else:
            if i == 0 and j < grid_y - 1:
                ways.append("y")
            if i < grid_x - 1:
                ways.append("x")
        return ways

    def came_along(place, color):
        i, j = place
        if color == 0:
            return ("y", (i, j - 1)) if j > 0 else ("x", (i - 1, j))
        return ("x", (i - 1, j)) if i > 0 else ("y", (i, j - 1))

    def stage(number, orders=(0, 1), parts=range(PIECES)):
        for order in orders:
            for part in parts:
                for place in places:
                    if sum(place) != number:
                        continue
                    for color in range(2):
                        if order == 0 and number > 0:
                            along, before = came_along(place, color)
                            block, landing = piece(place, color, part, core), slot(place, color, part)
                            pltpu.make_async_remote_copy(
                                src_ref=block,
                                dst_ref=block,
                                send_sem=ring_send.at[landing],
                                recv_sem=ring_recv.at[landing],
                                device_id={"fsdp": right_x},
                                device_id_type=MESH,
                            ).wait_recv()
                        ways = onward(place, color)
                        if order < len(ways):
                            ring_copy(place, color, part, ways[order]).start()
                        if order == 0:
                            core_copy(place, color, part, core).start()

    stage(0, (0,))
    for b in range(batch):
        load("q", b).start()
        load("g", b).start()

    leading = jnp.where(z < seq // 2, 0, 1)
    trailing = 1 - leading

    def has_in(d):
        return jnp.where(d == 0, z, seq - 1 - z) > 0

    def has_out(d):
        return jnp.where(d == 0, seq - 1 - z, z) > 0

    def state_copy(d, c):
        return pltpu.make_async_remote_copy(
            src_ref=gone.at[d, c],
            dst_ref=came.at[d, c],
            send_sem=state_send.at[d, c],
            recv_sem=state_recv.at[d, c],
            device_id={"seq": z + 1 - 2 * d},
            device_id_type=MESH,
        )

    def mass_copy(d, b):
        return pltpu.make_async_remote_copy(
            src_ref=gone_mass.at[d, b],
            dst_ref=came_mass.at[d, b],
            send_sem=mass_send.at[d, b],
            recv_sem=mass_recv.at[d, b],
            device_id={"seq": z + 1 - 2 * d},
            device_id_type=MESH,
        )

    def relay(d, c):
        b = c // turns

        @pl.when(lax.rem(c, turns) == 0)
        def _():
            @pl.when(has_in(d))
            def _():
                mass_copy(d, b).wait_recv()

            @pl.when(jnp.logical_not(has_in(d)))
            def _():
                came_mass[d, b] = jnp.zeros_like(came_mass[d, b])

            @pl.when(has_out(d))
            def _():
                gone_mass[d, b] = own_mass[b] + came_mass[d, b]
                mass_copy(d, b).start()

        @pl.when(has_in(d))
        def _():
            state_copy(d, c).wait_recv()

            @pl.when(has_out(d))
            def _():
                gone[d, c] = (own[c] + came[d, c].astype(jnp.float32)).astype(jnp.bfloat16)
                state_copy(d, c).start()

        @pl.when(jnp.logical_not(has_in(d)))
        def _():
            came[d, c] = jnp.zeros_like(came[d, c])

            @pl.when(has_out(d))
            def _():
                gone[d, c] = own[c].astype(jnp.bfloat16)
                state_copy(d, c).start()

    def group_of(o):
        i = j = 0
        for number, place in enumerate(places):
            i = jnp.where(o == number, place[0], i)
            j = jnp.where(o == number, place[1], j)
        return lax.rem(y - j + grid_y, grid_y) * grid_x + lax.rem(x - i + grid_x, grid_x)

    def head_of(c, n):
        order = lax.rem(c, turns) * together + n
        return group_of(order // group_heads) * group_heads + lax.rem(order, group_heads)

    step_tokens = 16

    def widen_kv(b):
        load("k", b).wait()
        load("v", b).wait()

        def body(n, mass):
            here = pl.ds(n * step_tokens, step_tokens)
            flat = pl.ds(pl.multiple_of(n * step_tokens * heads, step_tokens * heads), step_tokens * heads)
            feature = feature_map(k_raw[b, here].astype(jnp.float32)).astype(jnp.float32)
            k_wide[b, flat, :] = feature.reshape(step_tokens * heads, size)
            v_wide[b, flat, :] = v_raw[b, here].astype(jnp.float32).reshape(step_tokens * heads, size)
            return mass + jnp.sum(feature, axis=0)

        own_mass[b] = lax.fori_loop(0, tokens // step_tokens, body, jnp.zeros((heads, size), jnp.float32))

    def widen_qg(b):
        load("q", b).wait()
        load("g", b).wait()

        def body(n, carry):
            here = pl.ds(n * step_tokens, step_tokens)
            flat = pl.ds(pl.multiple_of(n * step_tokens * heads, step_tokens * heads), step_tokens * heads)
            q = q_raw[b, here].astype(jnp.float32)
            q_wide[b, flat, :] = (q * q + 0.1).reshape(step_tokens * heads, size)
            g = g_raw[b, here].astype(jnp.float32)
            g_wide[b, flat, :] = (count**0.5 / (1.0 + jnp.exp(-g))).reshape(step_tokens * heads, size)
            return carry

        lax.fori_loop(0, tokens // step_tokens, body, 0)

    def own_state(c, n):
        b, head = c // turns, head_of(c, n)
        feature = k_wide[b, pl.ds(head, tokens, stride=heads), :].astype(jnp.bfloat16)
        value = v_wide[b, pl.ds(head, tokens, stride=heads), :].astype(jnp.bfloat16)
        own[c, n] = lax.dot_general(
            value, feature, (((0,), (0,)), ((), ())), preferred_element_type=jnp.float32
        )

    def read(c, n):
        b, head = c // turns, head_of(c, n)
        state = own[c, n] + came[0, c, n].astype(jnp.float32) + came[1, c, n].astype(jnp.float32)
        one = pl.ds(head, 1)
        mass = own_mass[b, one] + came_mass[0, b, one] + came_mass[1, b, one]
        both = jnp.concatenate(
            [(state / count).astype(jnp.bfloat16), jnp.broadcast_to((mass / count).astype(jnp.bfloat16), state.shape)],
            axis=0,
        )
        feature = q_wide[b, pl.ds(head, tokens, stride=heads), :].astype(jnp.bfloat16)
        found = lax.dot_general(feature, both, (((1,), (1,)), ((), ())), preferred_element_type=jnp.float32)
        gate = g_wide[b, pl.ds(head, tokens, stride=heads), :]
        done = found[:, :size] / (found[:, size:] + 0.001) * gate
        columns = pl.ds(pl.multiple_of(head * size, size), size)
        mixed[pl.ds(pl.multiple_of(b * tokens, tokens), tokens), columns] = done.astype(jnp.bfloat16)

    def project(o):
        place = places[o]
        if sum(place) == last_stage and (o == 0 or sum(places[o - 1]) != last_stage):
            stage(last_stage, (0,), range(1, PIECES)) if last_stage > 0 else None
        last = o == len(places) - 1
        if last and rows % 128 == 0 and o > 0:
            project_part(o, group_of(o) * 2 * rows + core * rows, rows, False)
            arrived(place)
            project_part(o, group_of(o) * 2 * rows + (1 - core) * rows, rows, True)
        else:
            arrived(place)
            project_part(o, group_of(o) * 2 * rows, 2 * rows, last)

    def arrived(place):
        for color in range(2):
            for part in range(PIECES):
                core_copy(place, color, part, 1 - core).wait_recv()

    def project_part(o, start, deep, last):
        here = pl.ds(pl.multiple_of(start, deep), deep)

        def body(n, carry):
            columns = pl.ds(pl.multiple_of(n * COLUMN_TILE, COLUMN_TILE), COLUMN_TILE)
            term = jnp.dot(mixed[:, here], weight[here, columns], preferred_element_type=jnp.float32)
            if o > 0:
                term = total[:, columns] + term
            if not last:
                total[:, columns] = term
            else:
                for b in range(batch):
                    results[b][:, columns] = term[b * tokens : (b + 1) * tokens].astype(jnp.bfloat16)
            return carry

        lax.fori_loop(0, width // COLUMN_TILE, body, 0)

    nearer = jnp.minimum(z, seq - 1 - z)
    lead_lag = nearer * HOP_LAG
    trail_lag = (seq - 1 - nearer) * HOP_LAG

    def step(k, carry):
        late = k - trail_lag

        @pl.when(jnp.logical_and(k - lead_lag >= 0, k - lead_lag < chunks))
        def _():
            relay(leading, k - lead_lag)

        @pl.when(jnp.logical_and(late >= 0, late < chunks))
        def _():
            relay(trailing, late)

        @pl.when(k == SECOND_SIXTEENTHS * chunks // 16)
        def _():
            stage(0, (1,))

        for number in range(1, last_stage):
            @pl.when(k == number * STAGE_SIXTEENTHS * chunks // (16 * (last_stage - 1)))
            def _():
                stage(number)

        if last_stage > 0:
            pl.when(late == chunks - 1)(functools.partial(stage, last_stage, (0,), range(1)))

        later = k + 1

        @pl.when(jnp.logical_and(later < chunks, lax.rem(later, turns) == 0))
        def _():
            widen_kv(later // turns)

        @pl.when(later < chunks)
        def _():
            for n in range(together):
                own_state(later, n)

        @pl.when(jnp.logical_and(late + 1 >= 0, jnp.logical_and(late + 1 < chunks, lax.rem(late + 1, turns) == 0)))
        def _():
            widen_qg((late + 1) // turns)

        @pl.when(jnp.logical_and(late >= 0, late < chunks))
        def _():
            for n in range(together):
                read(late, n)

        for o in range(len(places)):
            @pl.when(late == chunks - turns + group_turns * (o + 1) - 1)
            def _():
                project(o)

        return carry

    widen_kv(0)
    for n in range(together):
        own_state(0, n)
    lax.fori_loop(0, chunks + (seq - 1) * HOP_LAG, step, 0)

    for place in places:
        for color in range(2):
            for part in range(PIECES):
                core_copy(place, color, part, core).wait_send()
                for along in onward(place, color):
                    ring_copy(place, color, part, along).wait_send()
    for d in range(2):

        @pl.when(has_out(d))
        def _():
            for b in range(batch):
                mass_copy(d, b).wait_send()

            def body(c, carry):
                state_copy(d, c).wait_send()
                return carry

            lax.fori_loop(0, chunks, body, 0)


def store(*refs):
    *parts, out, sem = refs
    copies = [pltpu.make_async_copy(part, out.at[b], sem.at[b]) for b, part in enumerate(parts)]
    for copy in copies:
        copy.start()
    for copy in copies:
        copy.wait()


def local(fsdp, seq, query_rows, key_rows, value_rows, gate_rows, out_weight):
    batch, tokens, heads, size = query_rows.shape
    rows, width = out_weight.shape
    grid_y, grid_x = chip_grid(fsdp)
    slots = grid_x * grid_y * 2 * PIECES
    together = math.gcd(CHUNK_HEADS, heads // (grid_x * grid_y))
    chunks = batch * heads // together
    raw = pltpu.VMEM(query_rows.shape, jnp.bfloat16)
    wide = pltpu.VMEM((batch, tokens * heads, size), jnp.float32)
    dma = pltpu.SemaphoreType.DMA
    parts = pl.pallas_call(
        functools.partial(kernel, fsdp, seq),
        out_shape=[jax.ShapeDtypeStruct((tokens, width), jnp.bfloat16)] * batch,
        in_specs=[pl.BlockSpec(memory_space=pl.ANY)] * 5,
        out_specs=[pl.BlockSpec(memory_space=pltpu.VMEM)] * batch,
        scratch_shapes=[
            raw,
            raw,
            raw,
            raw,
            wide,
            wide,
            wide,
            wide,
            pltpu.VMEM((chunks, together, size, size), jnp.float32),
            pltpu.VMEM((batch, heads, size), jnp.float32),
            pltpu.VMEM((2, chunks, together, size, size), jnp.bfloat16),
            pltpu.VMEM((2, chunks, together, size, size), jnp.bfloat16),
            pltpu.VMEM((2, batch, heads, size), jnp.float32),
            pltpu.VMEM((2, batch, heads, size), jnp.float32),
            pltpu.VMEM((rows * fsdp, width), jnp.bfloat16),
            pltpu.VMEM((batch * tokens, heads * size), jnp.bfloat16),
            pltpu.VMEM((batch * tokens, width), jnp.float32),
            dma((5, batch)),
            dma((2, chunks)),
            dma((2, chunks)),
            dma((2, batch)),
            dma((2, batch)),
            dma((slots,)),
            dma((slots,)),
            dma((slots,)),
            dma((slots,)),
        ],
        compiler_params=pltpu.CompilerParams(
            collective_id=0, has_side_effects=True, vmem_limit_bytes=VMEM_MIB * 1024 * 1024
        ),
        name="attend",
    )(query_rows, key_rows, value_rows, gate_rows, out_weight)
    return pl.pallas_call(
        store,
        out_shape=jax.ShapeDtypeStruct((batch, tokens, width), jnp.bfloat16),
        in_specs=[pl.BlockSpec(memory_space=pl.ANY)] * batch,
        out_specs=pl.BlockSpec(memory_space=pl.ANY),
        scratch_shapes=[dma((batch,))],
        compiler_params=pltpu.CompilerParams(vmem_limit_bytes=8 * 1024 * 1024),
        name="store",
    )(*parts)


def solution(mesh):
    row_spec = P("fsdp", "seq", None, None)
    return jax.shard_map(
        functools.partial(local, mesh.shape["fsdp"], mesh.shape["seq"]),
        mesh=mesh,
        in_specs=(row_spec, row_spec, row_spec, row_spec, P("fsdp", None)),
        out_specs=P("fsdp", "seq", None),
        check_vma=False,
    )
```

```python
import functools
import math

import jax
import jax.numpy as jnp
from jax import lax
from jax.experimental import pallas as pl
from jax.experimental.pallas import tpu as pltpu
from jax.sharding import PartitionSpec as P

MESH = pl.DeviceIdType.MESH
CHUNK_HEADS = 2
HOP_LAG = 3
STAGE_SIXTEENTHS = 16
SECOND_SIXTEENTHS = 6
VMEM_MIB = 52
PIECES = 2
COLUMN_TILE = 2048


def feature_map(wide):
    return (wide * wide + 0.1).astype(jnp.bfloat16)


def chip_grid(fsdp):
    chips = fsdp // 2
    along_x = max(size for size in range(1, math.isqrt(chips) + 1) if chips % size == 0)
    return chips // along_x, along_x


def kernel(
    fsdp,
    seq,
    q_hbm,
    k_hbm,
    v_hbm,
    g_hbm,
    w_hbm,
    *rest,
):
    results, rest = rest[: q_hbm.shape[0]], rest[q_hbm.shape[0] :]
    attend(fsdp, seq, q_hbm, k_hbm, v_hbm, g_hbm, w_hbm, results, *rest)


def attend(
    fsdp,
    seq,
    q_hbm,
    k_hbm,
    v_hbm,
    g_hbm,
    w_hbm,
    results,
    q_raw,
    k_raw,
    v_raw,
    g_raw,
    q_wide,
    k_wide,
    v_wide,
    g_wide,
    own,
    own_mass,
    came,
    gone,
    came_mass,
    gone_mass,
    weight,
    mixed,
    total,
    load_sem,
    state_send,
    state_recv,
    mass_send,
    mass_recv,
    ring_send,
    ring_recv,
    core_send,
    core_recv,
):
    batch, tokens, heads, size = q_raw.shape
    rows = w_hbm.shape[0]
    width = weight.shape[1]
    count = tokens * seq
    grid_y, grid_x = chip_grid(fsdp)
    group_heads = heads // (grid_x * grid_y)
    together = math.gcd(CHUNK_HEADS, group_heads)
    turns = heads // together
    group_turns = group_heads // together
    chunks = batch * turns
    places = sorted(
        ((i, j) for i in range(grid_x) for j in range(grid_y)), key=lambda place: (sum(place), place[1])
    )
    last_stage = grid_x + grid_y - 2

    f, z = lax.axis_index("fsdp"), lax.axis_index("seq")
    core, chip = lax.rem(f, 2), f // 2
    x, y = lax.rem(chip, grid_x), chip // grid_x

    def at(chip_y, chip_x, which):
        return (chip_y * grid_x + chip_x) * 2 + which

    right_x = at(y, lax.rem(x + 1, grid_x), core)
    right_y = at(lax.rem(y + 1, grid_y), x, core)
    other_core = at(y, x, 1 - core)

    loads = {}
    for number, (name, source, target) in enumerate(
        (("k", k_hbm, k_raw), ("v", v_hbm, v_raw), ("q", q_hbm, q_raw), ("g", g_hbm, g_raw))
    ):
        loads[name] = (source, target, number)

    def load(name, b):
        source, target, number = loads[name]
        return pltpu.make_async_copy(source.at[b], target.at[b], load_sem.at[number, b])

    own_rows = weight.at[pl.ds(pl.multiple_of(f * rows, rows), rows), :]
    load_weight = pltpu.make_async_copy(w_hbm, own_rows, load_sem.at[4, 0])
    load_weight.start()
    for b in range(batch):
        load("k", b).start()
        load("v", b).start()

    barrier = pltpu.get_barrier_semaphore()
    greeted = [{"fsdp": other_core}]
    if grid_x > 1:
        greeted.append({"fsdp": right_x})
    if grid_x > 2:
        greeted.append({"fsdp": at(y, lax.rem(x + grid_x - 1, grid_x), core)})
    if grid_y > 1:
        greeted.append({"fsdp": right_y})
    if grid_y > 2:
        greeted.append({"fsdp": at(lax.rem(y + grid_y - 1, grid_y), x, core)})
    for device in greeted:
        pl.semaphore_signal(barrier, inc=1, device_id=device, device_id_type=MESH)

    @pl.when(z > 0)
    def _():
        pl.semaphore_signal(barrier, inc=1, device_id={"seq": z - 1}, device_id_type=MESH)

    @pl.when(z < seq - 1)
    def _():
        pl.semaphore_signal(barrier, inc=1, device_id={"seq": z + 1}, device_id_type=MESH)

    ends = jnp.where(z > 0, 1, 0) + jnp.where(z < seq - 1, 1, 0)
    load_weight.wait()
    pl.semaphore_wait(barrier, len(greeted) + ends)

    piece_rows = rows // (2 * PIECES)

    def piece(place, color, part, which):
        i, j = place
        owner = at(lax.rem(y - j + grid_y, grid_y), lax.rem(x - i + grid_x, grid_x), which)
        start = owner * rows + (color * PIECES + part) * piece_rows
        return weight.at[pl.ds(pl.multiple_of(start, piece_rows), piece_rows), :]

    number_of = {place: number for number, place in enumerate(places)}

    def slot(place, color, part):
        return (number_of[place] * 2 + color) * PIECES + part

    def ring_copy(place, color, part, along):
        further = (place[0] + 1, place[1]) if along == "x" else (place[0], place[1] + 1)
        block, landing = piece(place, color, part, core), slot(further, color, part)
        return pltpu.make_async_remote_copy(
            src_ref=block,
            dst_ref=block,
            send_sem=ring_send.at[landing],
            recv_sem=ring_recv.at[landing],
            device_id={"fsdp": right_x if along == "x" else right_y},
            device_id_type=MESH,
        )

    def core_copy(place, color, part, which):
        block = piece(place, color, part, which)
        return pltpu.make_async_remote_copy(
            src_ref=block,
            dst_ref=block,
            send_sem=core_send.at[slot(place, color, part)],
            recv_sem=core_recv.at[slot(place, color, part)],
            device_id={"fsdp": other_core},
            device_id_type=MESH,
        )

    def onward(place, color):
        i, j = place
        ways = []
        if color == 0:
            if j == 0 and i < grid_x - 1:
                ways.append("x")
            if j < grid_y - 1:
                ways.append("y")
        else:
            if i == 0 and j < grid_y - 1:
                ways.append("y")
            if i < grid_x - 1:
                ways.append("x")
        return ways

    def came_along(place, color):
        i, j = place
        if color == 0:
            return ("y", (i, j - 1)) if j > 0 else ("x", (i - 1, j))
        return ("x", (i - 1, j)) if i > 0 else ("y", (i, j - 1))

    def stage(number, orders=(0, 1), parts=range(PIECES)):
        for order in orders:
            for part in parts:
                for place in places:
                    if sum(place) != number:
                        continue
                    for color in range(2):
                        if order == 0 and number > 0:
                            along, before = came_along(place, color)
                            block, landing = piece(place, color, part, core), slot(place, color, part)
                            pltpu.make_async_remote_copy(
                                src_ref=block,
                                dst_ref=block,
                                send_sem=ring_send.at[landing],
                                recv_sem=ring_recv.at[landing],
                                device_id={"fsdp": right_x},
                                device_id_type=MESH,
                            ).wait_recv()
                        ways = onward(place, color)
                        if order < len(ways):
                            ring_copy(place, color, part, ways[order]).start()
                        if order == 0:
                            core_copy(place, color, part, core).start()

    stage(0, (0,))
    for b in range(batch):
        load("q", b).start()
        load("g", b).start()

    leading = jnp.where(z < seq // 2, 0, 1)
    trailing = 1 - leading

    def has_in(d):
        return jnp.where(d == 0, z, seq - 1 - z) > 0

    def has_out(d):
        return jnp.where(d == 0, seq - 1 - z, z) > 0

    def state_copy(d, c):
        return pltpu.make_async_remote_copy(
            src_ref=gone.at[d, c],
            dst_ref=came.at[d, c],
            send_sem=state_send.at[d, c],
            recv_sem=state_recv.at[d, c],
            device_id={"seq": z + 1 - 2 * d},
            device_id_type=MESH,
        )

    def mass_copy(d, b):
        return pltpu.make_async_remote_copy(
            src_ref=gone_mass.at[d, b],
            dst_ref=came_mass.at[d, b],
            send_sem=mass_send.at[d, b],
            recv_sem=mass_recv.at[d, b],
            device_id={"seq": z + 1 - 2 * d},
            device_id_type=MESH,
        )

    def relay(d, c):
        b = c // turns

        @pl.when(lax.rem(c, turns) == 0)
        def _():
            @pl.when(has_in(d))
            def _():
                mass_copy(d, b).wait_recv()

            @pl.when(jnp.logical_not(has_in(d)))
            def _():
                came_mass[d, b] = jnp.zeros_like(came_mass[d, b])

            @pl.when(has_out(d))
            def _():
                gone_mass[d, b] = own_mass[b] + came_mass[d, b]
                mass_copy(d, b).start()

        @pl.when(has_in(d))
        def _():
            state_copy(d, c).wait_recv()

            @pl.when(has_out(d))
            def _():
                gone[d, c] = (own[c] + came[d, c].astype(jnp.float32)).astype(jnp.bfloat16)
                state_copy(d, c).start()

        @pl.when(jnp.logical_not(has_in(d)))
        def _():
            came[d, c] = jnp.zeros_like(came[d, c])

            @pl.when(has_out(d))
            def _():
                gone[d, c] = own[c].astype(jnp.bfloat16)
                state_copy(d, c).start()

    def group_of(o):
        i = j = 0
        for number, place in enumerate(places):
            i = jnp.where(o == number, place[0], i)
            j = jnp.where(o == number, place[1], j)
        return lax.rem(y - j + grid_y, grid_y) * grid_x + lax.rem(x - i + grid_x, grid_x)

    def head_of(c, n):
        order = lax.rem(c, turns) * together + n
        return group_of(order // group_heads) * group_heads + lax.rem(order, group_heads)

    step_tokens = 16

    def widen_kv(b):
        load("k", b).wait()
        load("v", b).wait()

        def body(n, mass):
            here = pl.ds(n * step_tokens, step_tokens)
            flat = pl.ds(pl.multiple_of(n * step_tokens * heads, step_tokens * heads), step_tokens * heads)
            feature = feature_map(k_raw[b, here].astype(jnp.float32)).astype(jnp.float32)
            k_wide[b, flat, :] = feature.reshape(step_tokens * heads, size)
            v_wide[b, flat, :] = v_raw[b, here].astype(jnp.float32).reshape(step_tokens * heads, size)
            return mass + jnp.sum(feature, axis=0)

        own_mass[b] = lax.fori_loop(0, tokens // step_tokens, body, jnp.zeros((heads, size), jnp.float32))

    def widen_qg(b):
        load("q", b).wait()
        load("g", b).wait()

        def body(n, carry):
            here = pl.ds(n * step_tokens, step_tokens)
            flat = pl.ds(pl.multiple_of(n * step_tokens * heads, step_tokens * heads), step_tokens * heads)
            q = q_raw[b, here].astype(jnp.float32)
            q_wide[b, flat, :] = (q * q + 0.1).reshape(step_tokens * heads, size)
            g = g_raw[b, here].astype(jnp.float32)
            g_wide[b, flat, :] = (count**0.5 / (1.0 + jnp.exp(-g))).reshape(step_tokens * heads, size)
            return carry

        lax.fori_loop(0, tokens // step_tokens, body, 0)

    def own_state(c, n):
        b, head = c // turns, head_of(c, n)
        feature = k_wide[b, pl.ds(head, tokens, stride=heads), :].astype(jnp.bfloat16)
        value = v_wide[b, pl.ds(head, tokens, stride=heads), :].astype(jnp.bfloat16)
        own[c, n] = lax.dot_general(
            value, feature, (((0,), (0,)), ((), ())), preferred_element_type=jnp.float32
        )

    def read(c, n):
        b, head = c // turns, head_of(c, n)
        state = own[c, n] + came[0, c, n].astype(jnp.float32) + came[1, c, n].astype(jnp.float32)
        one = pl.ds(head, 1)
        mass = own_mass[b, one] + came_mass[0, b, one] + came_mass[1, b, one]
        both = jnp.concatenate(
            [(state / count).astype(jnp.bfloat16), jnp.broadcast_to((mass / count).astype(jnp.bfloat16), state.shape)],
            axis=0,
        )
        feature = q_wide[b, pl.ds(head, tokens, stride=heads), :].astype(jnp.bfloat16)
        found = lax.dot_general(feature, both, (((1,), (1,)), ((), ())), preferred_element_type=jnp.float32)
        gate = g_wide[b, pl.ds(head, tokens, stride=heads), :]
        done = found[:, :size] / (found[:, size:] + 0.001) * gate
        columns = pl.ds(pl.multiple_of(head * size, size), size)
        mixed[pl.ds(pl.multiple_of(b * tokens, tokens), tokens), columns] = done.astype(jnp.bfloat16)

    def project(o):
        place = places[o]
        if sum(place) == last_stage and (o == 0 or sum(places[o - 1]) != last_stage):
            stage(last_stage, (0,), range(1, PIECES)) if last_stage > 0 else None
        last = o == len(places) - 1
        if last and rows % 128 == 0 and o > 0:
            project_part(o, group_of(o) * 2 * rows + core * rows, rows, False)
            arrived(place)
            project_part(o, group_of(o) * 2 * rows + (1 - core) * rows, rows, True)
        else:
            arrived(place)
            project_part(o, group_of(o) * 2 * rows, 2 * rows, last)

    def arrived(place):
        for color in range(2):
            for part in range(PIECES):
                core_copy(place, color, part, 1 - core).wait_recv()

    def project_part(o, start, deep, last):
        here = pl.ds(pl.multiple_of(start, deep), deep)

        def body(n, carry):
            columns = pl.ds(pl.multiple_of(n * COLUMN_TILE, COLUMN_TILE), COLUMN_TILE)
            term = jnp.dot(mixed[:, here], weight[here, columns], preferred_element_type=jnp.float32)
            if o > 0:
                term = total[:, columns] + term
            if not last:
                total[:, columns] = term
            else:
                for b in range(batch):
                    results[b][:, columns] = term[b * tokens : (b + 1) * tokens].astype(jnp.bfloat16)
            return carry

        lax.fori_loop(0, width // COLUMN_TILE, body, 0)

    nearer = jnp.minimum(z, seq - 1 - z)
    lead_lag = nearer * HOP_LAG
    trail_lag = (seq - 1 - nearer) * HOP_LAG

    def step(k, carry):
        late = k - trail_lag

        @pl.when(jnp.logical_and(k - lead_lag >= 0, k - lead_lag < chunks))
        def _():
            relay(leading, k - lead_lag)

        @pl.when(jnp.logical_and(late >= 0, late < chunks))
        def _():
            relay(trailing, late)

        @pl.when(k == SECOND_SIXTEENTHS * chunks // 16)
        def _():
            stage(0, (1,))

        for number in range(1, last_stage):
            @pl.when(k == number * STAGE_SIXTEENTHS * chunks // (16 * (last_stage - 1)))
            def _():
                stage(number)

        if last_stage > 0:
            pl.when(late == chunks - 1)(functools.partial(stage, last_stage, (0,), range(1)))

        later = k + 1

        @pl.when(jnp.logical_and(later < chunks, lax.rem(later, turns) == 0))
        def _():
            widen_kv(later // turns)

        @pl.when(later < chunks)
        def _():
            for n in range(together):
                own_state(later, n)

        @pl.when(jnp.logical_and(late + 1 >= 0, jnp.logical_and(late + 1 < chunks, lax.rem(late + 1, turns) == 0)))
        def _():
            widen_qg((late + 1) // turns)

        @pl.when(jnp.logical_and(late >= 0, late < chunks))
        def _():
            for n in range(together):
                read(late, n)

        for o in range(len(places)):
            @pl.when(late == chunks - turns + group_turns * (o + 1) - 1)
            def _():
                project(o)

        return carry

    widen_kv(0)
    for n in range(together):
        own_state(0, n)
    lax.fori_loop(0, chunks + (seq - 1) * HOP_LAG, step, 0)

    for place in places:
        for color in range(2):
            for part in range(PIECES):
                core_copy(place, color, part, core).wait_send()
                for along in onward(place, color):
                    ring_copy(place, color, part, along).wait_send()
    for d in range(2):

        @pl.when(has_out(d))
        def _():
            for b in range(batch):
                mass_copy(d, b).wait_send()

            def body(c, carry):
                state_copy(d, c).wait_send()
                return carry

            lax.fori_loop(0, chunks, body, 0)


def store(*refs):
    *parts, out, sem = refs
    copies = [pltpu.make_async_copy(part, out.at[b], sem.at[b]) for b, part in enumerate(parts)]
    for copy in copies:
        copy.start()
    for copy in copies:
        copy.wait()


def local(fsdp, seq, query_rows, key_rows, value_rows, gate_rows, out_weight):
    batch, tokens, heads, size = query_rows.shape
    rows, width = out_weight.shape
    grid_y, grid_x = chip_grid(fsdp)
    slots = grid_x * grid_y * 2 * PIECES
    together = math.gcd(CHUNK_HEADS, heads // (grid_x * grid_y))
    chunks = batch * heads // together
    raw = pltpu.VMEM(query_rows.shape, jnp.bfloat16)
    wide = pltpu.VMEM((batch, tokens * heads, size), jnp.float32)
    dma = pltpu.SemaphoreType.DMA
    parts = pl.pallas_call(
        functools.partial(kernel, fsdp, seq),
        out_shape=[jax.ShapeDtypeStruct((tokens, width), jnp.bfloat16)] * batch,
        in_specs=[pl.BlockSpec(memory_space=pl.ANY)] * 5,
        out_specs=[pl.BlockSpec(memory_space=pltpu.VMEM)] * batch,
        scratch_shapes=[
            raw,
            raw,
            raw,
            raw,
            wide,
            wide,
            wide,
            wide,
            pltpu.VMEM((chunks, together, size, size), jnp.float32),
            pltpu.VMEM((batch, heads, size), jnp.float32),
            pltpu.VMEM((2, chunks, together, size, size), jnp.bfloat16),
            pltpu.VMEM((2, chunks, together, size, size), jnp.bfloat16),
            pltpu.VMEM((2, batch, heads, size), jnp.float32),
            pltpu.VMEM((2, batch, heads, size), jnp.float32),
            pltpu.VMEM((rows * fsdp, width), jnp.bfloat16),
            pltpu.VMEM((batch * tokens, heads * size), jnp.bfloat16),
            pltpu.VMEM((batch * tokens, width), jnp.float32),
            dma((5, batch)),
            dma((2, chunks)),
            dma((2, chunks)),
            dma((2, batch)),
            dma((2, batch)),
            dma((slots,)),
            dma((slots,)),
            dma((slots,)),
            dma((slots,)),
        ],
        compiler_params=pltpu.CompilerParams(
            collective_id=0, has_side_effects=True, vmem_limit_bytes=VMEM_MIB * 1024 * 1024
        ),
        name="attend",
    )(query_rows, key_rows, value_rows, gate_rows, out_weight)
    return pl.pallas_call(
        store,
        out_shape=jax.ShapeDtypeStruct((batch, tokens, width), jnp.bfloat16),
        in_specs=[pl.BlockSpec(memory_space=pl.ANY)] * batch,
        out_specs=pl.BlockSpec(memory_space=pl.ANY),
        scratch_shapes=[dma((batch,))],
        compiler_params=pltpu.CompilerParams(vmem_limit_bytes=8 * 1024 * 1024),
        name="store",
    )(*parts)


def solution(mesh):
    row_spec = P("fsdp", "seq", None, None)
    return jax.shard_map(
        functools.partial(local, mesh.shape["fsdp"], mesh.shape["seq"]),
        mesh=mesh,
        in_specs=(row_spec, row_spec, row_spec, row_spec, P("fsdp", None)),
        out_specs=P("fsdp", "seq", None),
        check_vma=False,
    )
```
